512 devices in a mesh: dp: 128 (over x_lo, z, y), mp: 4 (over x_hi, core).
Axes of the slice: x: 4 (x_hi: 2, x_lo: 2; x = x_hi * 2 + x_lo), y: 8, z: 8, core: 2. Of those that a mesh axis runs over, the one named last changes fastest.
Arguments:
- hidden_input: bfloat16 [131072, 384], P('dp'), may hold values from -24 to 24
- output_cotangent: bfloat16 [131072, 8192], P('dp', 'mp'), may hold values from -0.023925781 to 0.023925781
- master_weights: float32 [384, 8192], P('dp', 'mp'), may hold values from -6 to 6
- first_codes: int32 [384, 8192], P('dp', 'mp'), may hold values from 0 to 15
- second_codes: int32 [384, 8192], P('dp', 'mp'), may hold values from 0 to 15
- first_rows: float32 [384], P('dp'), may hold values from 0.001 to 0.03
- first_cols: float32 [8192], P('mp'), may hold values from 0.001 to 0.03
- second_rows: float32 [384], P('dp'), may hold values from 1e-05 to 0.001
- second_cols: float32 [8192], P('mp'), may hold values from 1e-05 to 0.001
- step_count: int32 [], replicated, may hold values from 1 to 9
Outputs:
- new_master: float32 [384, 8192], P('dp', 'mp')
- update_ratio: float32 [384, 8192], P('dp', 'mp')
- gathered_params: bfloat16 [384, 8192], P(None, 'mp')
- first_scaled: float32 [384, 8192], P('dp', 'mp')
- second_scaled: float32 [384, 8192], P('dp', 'mp')
- new_first_rows: float32 [384], P('dp')
- new_first_cols: float32 [8192], P('mp')
- new_second_rows: float32 [384], P('dp')
- new_second_cols: float32 [8192], P('mp')
The draws below stay inside these ranges and needn't reach their ends.
All inputs are finite; a program needn't handle non-finite values.
Results may differ from the reference program's by a relative error of at most 0.001.
Values may be sent and summed in bfloat16 or wider, within the bound.
A program may use at most 64 MiB of HBM per device.

```python
import math
import jax
import jax.numpy as jnp
from jax import lax

D = 8192
ROWS = 384
TOKENS = 131072


def plant(values, own_key, low, high):
    longest = values.shape.index(max(values.shape))
    spots = []
    for shift in (0, 1):
        where = [jax.random.randint(jax.random.fold_in(own_key, axis), (), 0, length) for axis, length in enumerate(values.shape)]
        where[longest] = (where[longest] + shift) % values.shape[longest]
        spots.append(tuple(where))
    return values.at[spots[0]].set(low).at[spots[1]].set(high)


def spiked(values, own_key, source, target, parts, factor):
    def block_of(axis_at):
        return (jnp.arange(values.shape[axis_at]) // (values.shape[axis_at] // parts)).reshape((-1,) + (1,) * (values.ndim - 1 - axis_at))

    one_side = jax.random.permutation(own_key, parts)[block_of(target)]
    far = (block_of(target) + parts // 2) % parts
    return jnp.where((block_of(source) == one_side) | (block_of(source) == far), factor * values, values)


def block_scale(key, extent, pieces, smallest, high):
    loudness, own = 1.0, jax.random.fold_in(key, 6)
    for axis_at, parts in pieces:
        draws = jnp.exp(jax.random.uniform(jax.random.fold_in(own, axis_at), (parts,), jnp.float32, smallest / len(pieces), high / len(pieces)))
        loudness = loudness * jnp.repeat(draws, extent[axis_at] // parts).reshape([-1 if axis == axis_at else 1 for axis in range(len(extent))])
    return loudness


def bell_draw(stream_key, dims, deviation, most, split=(), kind=jnp.bfloat16):
    values = jax.random.normal(stream_key, dims, jnp.float32) * deviation
    if len(split) > 0:
        values = block_scale(stream_key, dims, split, -0.22, 0.18) * values
    return jnp.clip(values, min=-most, max=most).astype(kind)


def noise_with(own_key, extent, deviation, reach, shards, heavy, dtype=jnp.bfloat16):
    result = deviation * jax.random.normal(own_key, extent, jnp.float32)
    if shards:
        result = result * block_scale(own_key, extent, shards, -0.22, 0.18)
    return jnp.clip(spiked(result, jax.random.fold_in(own_key, 3), *heavy), -reach, reach).astype(dtype)


def setup_inputs(seed: int = 0) -> dict:
    splits = jax.random.split(jax.random.key(seed), 11)
    return {
        "hidden_input": noise_with(splits[0], (TOKENS, ROWS), 1.0, 24.0, ((0, 128),), (0, 1, 128, 5.5)),
        "output_cotangent": bell_draw(splits[1], (TOKENS, D), 0.004, 0.023925781, ((0, 128), (1, 4))),
        "master_weights": bell_draw(splits[2], (ROWS, D), 1.0, 6.0, ((0, 128), (1, 4)), jnp.float32),
        "first_codes": plant(jax.random.randint(splits[3], (ROWS, D), 0, 16), jax.random.fold_in(splits[3], 1), 0, 15).astype(jnp.int32),
        "second_codes": plant(jax.random.randint(splits[4], (ROWS, D), 0, 16), jax.random.fold_in(splits[4], 1), 0, 15).astype(jnp.int32),
        "first_rows": jnp.clip(jnp.exp(math.log(0.03) - 3.4011973 * jax.random.uniform(splits[5], (ROWS,), jnp.float32) ** block_scale(splits[5], (ROWS,), ((0, 128),), -0.2, 0.2)), 0.001, 0.03),
        "first_cols": jnp.clip(jnp.exp(math.log(0.03) - 3.4011973 * jax.random.uniform(splits[6], (D,), jnp.float32) ** block_scale(splits[6], (D,), ((0, 4),), -0.2, 0.2)), 0.001, 0.03),
        "second_rows": jnp.clip(jnp.exp(math.log(0.001) - 4.6051703 * jax.random.uniform(splits[7], (ROWS,), jnp.float32) ** block_scale(splits[7], (ROWS,), ((0, 128),), -0.2, 0.2)), 9.999999747378752e-06, 0.001),
        "second_cols": jnp.clip(jnp.exp(math.log(0.001) - 4.6051703 * jax.random.uniform(splits[8], (D,), jnp.float32) ** block_scale(splits[8], (D,), ((0, 4),), -0.2, 0.2)), 9.999999747378752e-06, 0.001),
        "step_count": jax.random.randint(splits[9], (), 1, 10).astype(jnp.int32),
    }


def reference(hidden_input, output_cotangent, master_weights, first_codes, second_codes, first_rows, first_cols, second_rows, second_cols, step_count):
    gradient = jnp.dot(hidden_input.T, output_cotangent, preferred_element_type=jnp.float32)
    entries = gradient.shape[0] * gradient.shape[1]
    gnorm = jnp.sqrt(jnp.sum(gradient * gradient))
    clipf = jnp.minimum(1.0, 0.01 * jnp.sqrt(jnp.float32(entries)) / (gnorm + 1e-06))
    clipped = clipf * gradient
    first_old = (first_codes.astype(jnp.float32) - 7.5) / 7.5 * jnp.minimum(first_rows[:, None], first_cols[None, :])
    second_level = (second_codes.astype(jnp.float32) + 1.0) / 16.0
    second_old = second_level * second_level * jnp.minimum(second_rows[:, None], second_cols[None, :])
    first_new = 0.9 * first_old + 0.1 * clipped
    second_new = 0.95 * second_old + 0.05 * clipped * clipped
    steps = step_count.astype(jnp.float32)
    first_fix = 1.0 - jnp.power(jnp.float32(0.9), steps)
    second_fix = 1.0 - jnp.power(jnp.float32(0.95), steps)
    update_ratio = first_new / first_fix / (jnp.sqrt(second_new / second_fix) + 1e-08)
    new_master = master_weights - 0.001 * (update_ratio + 0.1 * master_weights)
    first_abs = jnp.abs(first_new)
    new_first_rows = lax.optimization_barrier(jnp.max(first_abs, axis=1))
    new_first_cols = lax.optimization_barrier(jnp.max(first_abs, axis=0))
    new_second_rows = lax.optimization_barrier(jnp.max(second_new, axis=1))
    new_second_cols = lax.optimization_barrier(jnp.max(second_new, axis=0))
    first_scaled = first_new / (jnp.minimum(new_first_rows[:, None], new_first_cols[None, :]) + 1e-08)
    second_scaled = second_new / (jnp.minimum(new_second_rows[:, None], new_second_cols[None, :]) + 1e-08)
    gathered_params = new_master.astype(jnp.bfloat16)
    return (new_master, update_ratio, gathered_params, first_scaled, second_scaled, new_first_rows, new_first_cols, new_second_rows, new_second_cols)
```

```python
import jax
import jax.numpy as jnp
import numpy as np
from jax import lax
from jax.experimental import pallas as pl
from jax.experimental.pallas import tpu as pltpu
from jax.sharding import Mesh
from jax.sharding import PartitionSpec as P

DP = ("dp_0", "dp_1", "dp_2")
MP = ("mp_0", "mp_1")
MESH = pl.DeviceIdType.MESH
F32, BF16, I16, I32 = jnp.float32, jnp.bfloat16, jnp.int16, jnp.int32

RING = 8
PLANE = 16
OWN = 3
CHUNK = PLANE * OWN
ROWS = RING * CHUNK
COLS = 2048
WIDTH = 512
BLOCKS = 4
TOKENS = 1024
ORDER = (2, 0, 3, 1)
TOP = 32767.0


def along_y(b):
    return b < 2


def long_way(b):
    return 1 if b % 2 else -1


def kernel(
    hid,
    cot,
    master,
    codes1,
    codes2,
    rows1,
    cols1,
    rows2,
    cols2,
    step,
    perm,
    back_y,
    back_z,
    out_master,
    out_ratio,
    out_params,
    out_scaled1,
    out_scaled2,
    out_rows1,
    out_cols1,
    out_rows2,
    out_cols2,
    hid_v,
    cot_v,
    perm_v,
    back_v,
    hid_t,
    grad,
    ship,
    ship_scale,
    land,
    land_scale,
    total,
    piece_out,
    piece_in,
    norm_out,
    norm_in,
    fresh,
    near,
    join,
    whole,
    natural,
    col_out,
    col_in,
    row_out,
    row_in,
    local_sem,
    out_sem,
    ring_send,
    ring_recv,
    scale_send,
    scale_recv,
    plane_send,
    plane_recv,
    norm_send,
    norm_recv,
    near_send,
    near_recv,
    whole_send,
    whole_recv,
    col_send,
    col_recv,
    row_send,
    row_recv,
):
    xl = lax.axis_index("dp_0")
    z = lax.axis_index("dp_1")
    y = lax.axis_index("dp_2")
    xh = lax.axis_index("mp_0")
    core = lax.axis_index("mp_1")
    plane_z = xl * 8 + z
    plane_y = xl * 8 + y
    cube = xl * 4 + xh * 2 + core
    quad = xh * 2 + core

    def in_plane(b, k):
        return {"dp_0": k // 8, ("dp_1" if along_y(b) else "dp_2"): k % 8}

    def in_plane_z(k):
        return {"dp_0": k // 8, "dp_1": k % 8}

    def my_place(b):
        return plane_z if along_y(b) else plane_y

    def on_ring(b, c):
        return {("dp_2" if along_y(b) else "dp_1"): lax.rem(c + 16, 8)}

    def my_ring(b):
        return y if along_y(b) else z

    def in_cube(k):
        return {"dp_0": k // 4, "mp_0": (k // 2) % 2, "mp_1": k % 2}

    def in_quad(k):
        return {"mp_0": k // 2, "mp_1": k % 2}

    def remote(src, dst, send, recv, where):
        return pltpu.make_async_remote_copy(
            src_ref=src,
            dst_ref=dst,
            send_sem=send,
            recv_sem=recv,
            device_id=where,
            device_id_type=MESH,
        )

    def each_other(count, me, act):
        def body(i, carry):
            act(lax.rem(me + i, count))
            return carry

        lax.fori_loop(1, count, body, 0)

    def bytes_of(ref, sem):
        pltpu.make_async_copy(ref, ref, sem).wait()

    barrier = pltpu.get_barrier_semaphore()

    def greet(where):
        pl.semaphore_signal(barrier, inc=1, device_id=where, device_id_type=MESH)

    each_other(16, plane_z, lambda k: greet(in_plane_z(k)))

    def greet_y(i, carry):
        other = lax.rem(y + i, 8)
        greet({"dp_2": other})
        greet({"dp_0": 1 - xl, "dp_2": other})
        return carry

    lax.fori_loop(1, 8, greet_y, 0)

    def greet_mp(i, carry):
        k = lax.rem(quad + i, 4)
        greet(in_quad(k))
        greet({"dp_0": 1 - xl, "mp_0": k // 2, "mp_1": k % 2})
        return carry

    lax.fori_loop(1, 4, greet_mp, 0)

    hid_copy = pltpu.make_async_copy(hid, hid_v, local_sem.at[4])
    hid_copy.start()
    cot_copies = {}
    for b in ORDER:
        cot_copies[b] = pltpu.make_async_copy(
            cot.at[:, pl.ds(b * WIDTH, WIDTH)], cot_v.at[b], local_sem.at[b]
        )
    cot_copies[ORDER[0]].start()
    perm_copy = pltpu.make_async_copy(perm, perm_v, local_sem.at[5])
    perm_copy.start()
    for b in ORDER[1:]:
        cot_copies[b].start()
    back_copies = [
        pltpu.make_async_copy(back_y, back_v.at[0], local_sem.at[6]),
        pltpu.make_async_copy(back_z, back_v.at[1], local_sem.at[7]),
    ]
    for copy in back_copies:
        copy.start()

    ring_copies = {}

    def send_ring(b, slot, way, value):
        peak = jnp.maximum(jnp.max(jnp.abs(value), axis=0, keepdims=True), 1e-30)
        ship_scale[b, slot] = peak * (1.0 / TOP)
        coded = jnp.round(value * (TOP / peak))
        ship[b, slot] = coded.astype(I32).astype(I16)
        where = on_ring(b, my_ring(b) + way)
        data = remote(
            ship.at[b, slot], land.at[b, slot], ring_send.at[b], ring_recv.at[b, slot], where
        )
        scale = remote(
            ship_scale.at[b, slot],
            land_scale.at[b, slot],
            scale_send.at[b],
            scale_recv.at[b, slot],
            where,
        )
        data.start()
        scale.start()
        ring_copies[b, slot] = (data, scale)

    def arrived(b, slot):
        data, scale = ring_copies[b, slot]
        data.wait_recv()
        scale.wait_recv()
        return land[b, slot].astype(I32).astype(F32) * land_scale[b, slot]

    def own(b, c):
        return grad[b, lax.rem(c + 16, 8)]

    def first_sends(b):
        me, way = my_ring(b), long_way(b)
        send_ring(b, 0, way, own(b, me + 4))
        send_ring(b, 4, -way, own(b, me - 3 * way))

    hid_copy.wait()
    hid_t[1] = hid_v[...].T
    ready = False
    for b in ORDER:
        if b == ORDER[1]:
            perm_copy.wait()
            hid_t[0] = jnp.dot(perm_v[...], hid_t[1], preferred_element_type=F32).astype(BF16)
        cot_copies[b].wait()
        lhs = hid_t[0] if along_y(b) else hid_t[1]
        product = jnp.dot(lhs, cot_v[b], preferred_element_type=F32)
        if along_y(b):
            grad[b] = product.reshape(RING, CHUNK, WIDTH)
        else:
            half = CHUNK // 2
            grad[b, :, 0:half] = product[0 : ROWS // 2].reshape(RING, half, WIDTH)
            grad[b, :, half:CHUNK] = product[ROWS // 2 :].reshape(RING, half, WIDTH)
        if not ready:
            pl.semaphore_wait(barrier, 15 + 14 + 6)
            ready = True
        first_sends(b)

    for s in (1, 2):
        for b in ORDER:
            me, way = my_ring(b), long_way(b)
            send_ring(b, s, way, arrived(b, s - 1) + own(b, me + way * (4 - s)))
            send_ring(b, 4 + s, -way, arrived(b, 3 + s) + own(b, me - way * (3 - s)))
    for b in ORDER:
        me, way = my_ring(b), long_way(b)
        send_ring(b, 3, way, arrived(b, 2) + own(b, me + way))
        total[b] = arrived(b, 6) + own(b, me)
    for b in ORDER:
        total[b] += arrived(b, 3)
        for k in range(PLANE):
            piece_out[b, k] = total[b, OWN * k : OWN * k + OWN]
        mine = my_place(b)
        piece_in[b, mine] = piece_out[b, mine]

        def send_piece(k, b=b, mine=mine):
            remote(
                piece_out.at[b, k],
                piece_in.at[b, mine],
                plane_send.at[b],
                plane_recv.at[b],
                in_plane(b, k),
            ).start()

        each_other(PLANE, mine, send_piece)

    def as_column(ref):
        at = lax.broadcasted_iota(I32, (OWN, 1), 0)
        return jnp.where(at == 0, ref[0], jnp.where(at == 1, ref[1], ref[2]))

    first_old = (
        (codes1[...].astype(F32) - 7.5) / 7.5 * jnp.minimum(as_column(rows1), cols1[...])
    )
    level = (codes2[...].astype(F32) + 1.0) / 16.0
    second_old = level * level * jnp.minimum(as_column(rows2), cols2[...])
    steps = jnp.full((1, 128), step[0].astype(F32))
    first_fix = (1.0 - jnp.exp(steps * np.float32(np.log(0.9))))[:, 0:1]
    second_fix = (1.0 - jnp.exp(steps * np.float32(np.log(0.95))))[:, 0:1]

    parts = []
    for b in ORDER:
        bytes_of(piece_in.at[b, pl.ds(0, PLANE - 1)], plane_recv.at[b])
        parts.append((b, jnp.sum(piece_in[b], axis=0)))
    parts = dict(parts)
    gradient = jnp.concatenate([parts[b] for b in range(BLOCKS)], axis=1)

    square = jnp.sum(jnp.sum(gradient * gradient, axis=1, keepdims=True), axis=0, keepdims=True)
    square = jnp.broadcast_to(square, (1, 128))
    for phase, (me, to) in enumerate(
        ((y, lambda k: {"dp_2": k}), (z, lambda k: {"dp_1": k}), (cube, in_cube))
    ):
        norm_out[phase] = square
        norm_in[phase, me] = square

        def send_norm(k, phase=phase, me=me, to=to):
            remote(
                norm_out.at[phase],
                norm_in.at[phase, me],
                norm_send.at[phase],
                norm_recv.at[phase],
                to(k),
            ).start()

        each_other(8, me, send_norm)
        bytes_of(norm_in.at[phase, pl.ds(0, 7)], norm_recv.at[phase])
        square = jnp.sum(norm_in[phase], axis=0)

    entries = np.float32(3145728.0)
    limit = np.float32(0.01) * np.sqrt(entries)
    clipf = jnp.minimum(1.0, limit / (jnp.sqrt(square) + 1e-06))[:, 0:1]
    clipped = clipf * gradient
    first_new = 0.9 * first_old + 0.1 * clipped
    second_new = 0.95 * second_old + 0.05 * clipped * clipped
    ratio = first_new / first_fix / (jnp.sqrt(second_new / second_fix) + 1e-08)
    new_master = master[...] - 0.001 * (ratio + 0.1 * master[...])
    out_ratio[...] = ratio
    out_master[...] = new_master

    rounded = new_master.astype(BF16)
    for b in ORDER:
        mine = my_place(b)
        fresh[b] = rounded[:, b * WIDTH : (b + 1) * WIDTH]
        near[b, mine] = rounded[:, b * WIDTH : (b + 1) * WIDTH]

        def send_near(k, b=b, mine=mine):
            remote(
                fresh.at[b], near.at[b, mine], near_send.at[b], near_recv.at[b], in_plane(b, k)
            ).start()

        each_other(PLANE, mine, send_near)

    first_abs = jnp.abs(first_new)
    row_out[0] = jnp.broadcast_to(jnp.max(first_abs, axis=1, keepdims=True), (OWN, 128))
    row_out[1] = jnp.broadcast_to(jnp.max(second_new, axis=1, keepdims=True), (OWN, 128))
    row_in[quad] = row_out[...]
    each_other(
        4,
        quad,
        lambda k: remote(row_out, row_in.at[quad], row_send, row_recv, in_quad(k)).start(),
    )
    tops = jnp.concatenate(
        [jnp.max(first_abs, axis=0, keepdims=True), jnp.max(second_new, axis=0, keepdims=True)],
        axis=0,
    )
    for k in range(PLANE):
        col_out[0, k] = tops[:, 128 * k : 128 * k + 128]
    col_in[0, plane_z] = col_out[0, plane_z]
    each_other(
        PLANE,
        plane_z,
        lambda k: remote(
            col_out.at[0, k],
            col_in.at[0, plane_z],
            col_send.at[0],
            col_recv.at[0],
            in_plane_z(k),
        ).start(),
    )

    whole_copies = {}

    def pass_on(b, slot, way, c):
        at = lax.rem(c + 16, 8)
        copy = remote(
            whole.at[b, at],
            whole.at[b, at],
            whole_send.at[b],
            whole_recv.at[b, slot],
            on_ring(b, my_ring(b) + way),
        )
        copy.start()
        whole_copies[b, slot] = copy

    for b in ORDER:
        me, way = my_ring(b), long_way(b)
        bytes_of(near.at[b, pl.ds(0, PLANE - 1)], near_recv.at[b])
        for k in range(PLANE):
            join[b, OWN * k : OWN * k + OWN] = near[b, k].astype(F32)
        whole[b, me] = join[b].astype(BF16)
        pass_on(b, 0, way, me)
        pass_on(b, 4, -way, me)

    bytes_of(col_in.at[0, pl.ds(0, PLANE - 1)], col_recv.at[0])
    best = jnp.max(col_in[0], axis=0)
    col_out[1, 0] = best
    col_in[1, y] = best
    each_other(
        8,
        y,
        lambda k: remote(
            col_out.at[1, 0], col_in.at[1, y], col_send.at[1], col_recv.at[1], {"dp_2": k}
        ).start(),
    )

    def step_on(s):
        for b in ORDER:
            me, way = my_ring(b), long_way(b)
            whole_copies[b, s - 1].wait_recv()
            pass_on(b, s, way, me - way * s)
            if s < 3:
                whole_copies[b, 3 + s].wait_recv()
                pass_on(b, 4 + s, -way, me + way * s)

    step_on(1)
    bytes_of(col_in.at[1, pl.ds(0, 7)], col_recv.at[1])
    best = jnp.max(col_in[1, 0:8], axis=0)
    col_out[2, 0] = best
    col_in[2, plane_z] = best
    each_other(
        PLANE,
        plane_z,
        lambda k: remote(
            col_out.at[2, 0], col_in.at[2, plane_z], col_send.at[2], col_recv.at[2], in_plane_z(k)
        ).start(),
    )
    step_on(2)

    bytes_of(row_in.at[pl.ds(0, 3)], row_recv)
    row_top = jnp.max(row_in[...], axis=0)
    for j in range(OWN):
        out_rows1[j] = jnp.max(row_top[0, j : j + 1])
        out_rows2[j] = jnp.max(row_top[1, j : j + 1])
    step_on(3)

    bytes_of(col_in.at[2, pl.ds(0, PLANE - 1)], col_recv.at[2])
    for k in range(PLANE):
        out_cols1[:, 128 * k : 128 * k + 128] = col_in[2, k, 0:1]
        out_cols2[:, 128 * k : 128 * k + 128] = col_in[2, k, 1:2]
    out_scaled1[...] = first_new / (jnp.minimum(row_top[0, :, 0:1], out_cols1[...]) + 1e-08)
    out_scaled2[...] = second_new / (jnp.minimum(row_top[1, :, 0:1], out_cols2[...]) + 1e-08)

    for copy in back_copies:
        copy.wait()
    out_copies = []
    for b in ORDER:
        whole_copies[b, 3].wait_recv()
        whole_copies[b, 6].wait_recv()
        natural[b] = jnp.dot(
            back_v[0 if along_y(b) else 1],
            whole[b].reshape(ROWS, WIDTH),
            preferred_element_type=F32,
        ).astype(BF16)
        copy = pltpu.make_async_copy(
            natural.at[b], out_params.at[:, pl.ds(b * WIDTH, WIDTH)], out_sem.at[b]
        )
        copy.start()
        out_copies.append(copy)

    for b in range(BLOCKS):
        bytes_of(ship.at[b], ring_send.at[b])
        bytes_of(ship_scale.at[b], scale_send.at[b])
        bytes_of(piece_out.at[b, pl.ds(0, PLANE - 1)], plane_send.at[b])
        bytes_of(near.at[b, pl.ds(0, PLANE - 1)], near_send.at[b])
        bytes_of(whole.at[b, pl.ds(0, 7)], whole_send.at[b])
    for phase in range(3):
        bytes_of(norm_in.at[phase, pl.ds(0, 7)], norm_send.at[phase])
        bytes_of(
            col_in.at[phase, pl.ds(0, 7 if phase == 1 else PLANE - 1)], col_send.at[phase]
        )
    bytes_of(row_in.at[pl.ds(0, 3)], row_send)
    for copy in out_copies:
        copy.wait()


def permutations():
    natural = np.arange(ROWS)
    by_y = natural.reshape(PLANE, RING, OWN).transpose(1, 0, 2).reshape(-1)
    by_z = natural.reshape(2, RING, RING, OWN).transpose(1, 0, 2, 3).reshape(-1)
    to_y = np.zeros((ROWS, ROWS), np.float32)
    to_y[natural, by_y] = 1.0
    to_z = np.zeros((ROWS, ROWS), np.float32)
    to_z[natural, by_z] = 1.0
    return to_y, to_y.T, to_z.T


def shards(
    hidden_input,
    output_cotangent,
    master_weights,
    first_codes,
    second_codes,
    first_rows,
    first_cols,
    second_rows,
    second_cols,
    step_count,
):
    own = jax.ShapeDtypeStruct((OWN, COLS), F32)
    row = jax.ShapeDtypeStruct((OWN,), F32)
    col = jax.ShapeDtypeStruct((1, COLS), F32)
    anywhere = pl.BlockSpec(memory_space=pl.ANY)
    vmem = pl.BlockSpec(memory_space=pltpu.VMEM)
    smem = pl.BlockSpec(memory_space=pltpu.SMEM)
    dma = pltpu.SemaphoreType.DMA
    outs = pl.pallas_call(
        kernel,
        out_shape=(
            own,
            own,
            jax.ShapeDtypeStruct((ROWS, COLS), BF16),
            own,
            own,
            row,
            col,
            row,
            col,
        ),
        in_specs=[
            anywhere,
            anywhere,
            vmem,
            vmem,
            vmem,
            smem,
            vmem,
            smem,
            vmem,
            smem,
            anywhere,
            anywhere,
            anywhere,
        ],
        out_specs=(vmem, vmem, anywhere, vmem, vmem, smem, vmem, smem, vmem),
        scratch_shapes=[
            pltpu.VMEM((TOKENS, ROWS), BF16),
            pltpu.VMEM((BLOCKS, TOKENS, WIDTH), BF16),
            pltpu.VMEM((ROWS, ROWS), BF16),
            pltpu.VMEM((2, ROWS, ROWS), BF16),
            pltpu.VMEM((2, ROWS, TOKENS), BF16),
            pltpu.VMEM((BLOCKS, RING, CHUNK, WIDTH), F32),
            pltpu.VMEM((BLOCKS, 7, CHUNK, WIDTH), I16),
            pltpu.VMEM((BLOCKS, 7, 1, WIDTH), F32),
            pltpu.VMEM((BLOCKS, 7, CHUNK, WIDTH), I16),
            pltpu.VMEM((BLOCKS, 7, 1, WIDTH), F32),
            pltpu.VMEM((BLOCKS, CHUNK, WIDTH), F32),
            pltpu.VMEM((BLOCKS, PLANE, OWN, WIDTH), F32),
            pltpu.VMEM((BLOCKS, PLANE, OWN, WIDTH), F32),
            pltpu.VMEM((3, 1, 128), F32),
            pltpu.VMEM((3, 8, 1, 128), F32),
            pltpu.VMEM((BLOCKS, OWN, WIDTH), BF16),
            pltpu.VMEM((BLOCKS, PLANE, OWN, WIDTH), BF16),
            pltpu.VMEM((BLOCKS, CHUNK, WIDTH), F32),
            pltpu.VMEM((BLOCKS, RING, CHUNK, WIDTH), BF16),
            pltpu.VMEM((BLOCKS, ROWS, WIDTH), BF16),
            pltpu.VMEM((3, PLANE, 2, 128), F32),
            pltpu.VMEM((3, PLANE, 2, 128), F32),
            pltpu.VMEM((2, OWN, 128), F32),
            pltpu.VMEM((4, 2, OWN, 128), F32),
            dma((8,)),
            dma((BLOCKS,)),
            dma((BLOCKS,)),
            dma((BLOCKS, 7)),
            dma((BLOCKS,)),
            dma((BLOCKS, 7)),
            dma((BLOCKS,)),
            dma((BLOCKS,)),
            dma((3,)),
            dma((3,)),
            dma((BLOCKS,)),
            dma((BLOCKS,)),
            dma((BLOCKS,)),
            dma((BLOCKS, 7)),
            dma((3,)),
            dma((3,)),
            dma,
            dma,
        ],
        compiler_params=pltpu.CompilerParams(
            collective_id=0, has_side_effects=True, vmem_limit_bytes=56 * 1024 * 1024
        ),
    )(
        hidden_input,
        output_cotangent,
        master_weights,
        first_codes,
        second_codes,
        first_rows,
        first_cols.reshape(1, -1),
        second_rows,
        second_cols.reshape(1, -1),
        step_count.reshape(1),
        *(jnp.asarray(p, BF16) for p in permutations()),
    )
    outs = list(outs)
    outs[6] = outs[6].reshape(-1)
    outs[8] = outs[8].reshape(-1)
    return tuple(outs)


def solution(mesh):
    finer = Mesh(mesh.devices.reshape(2, 8, 8, 2, 2), ("dp_0", "dp_1", "dp_2", "mp_0", "mp_1"))
    in_specs = (
        P(DP, None),
        P(DP, MP),
        P(DP, MP),
        P(DP, MP),
        P(DP, MP),
        P(DP),
        P(MP),
        P(DP),
        P(MP),
        P(),
    )
    out_specs = (
        P(DP, MP),
        P(DP, MP),
        P(None, MP),
        P(DP, MP),
        P(DP, MP),
        P(DP),
        P(MP),
        P(DP),
        P(MP),
    )
    return jax.shard_map(
        shards, mesh=finer, in_specs=in_specs, out_specs=out_specs, check_vma=False
    )
```

```python
import jax
import jax.numpy as jnp
import numpy as np
from jax import lax
from jax.experimental import pallas as pl
from jax.experimental.pallas import tpu as pltpu
from jax.sharding import Mesh
from jax.sharding import PartitionSpec as P

DP = ("dp_0", "dp_1", "dp_2")
MP = ("mp_0", "mp_1")
MESH = pl.DeviceIdType.MESH
F32, BF16, I16, I32 = jnp.float32, jnp.bfloat16, jnp.int16, jnp.int32

RING = 8
PLANE = 16
OWN = 3
CHUNK = PLANE * OWN
ROWS = RING * CHUNK
COLS = 2048
WIDTH = 256
BLOCKS = 8
HALF = 1024
PART = 512
PARTS = 4
TOKENS = 1024
TOP = 32767.0


def long_way(b):
    return 1 if b % 2 else -1


def kernel(
    hid,
    cot,
    master,
    codes1,
    codes2,
    rows1,
    cols1,
    rows2,
    cols2,
    step,
    perm,
    out_master,
    out_ratio,
    out_whole,
    out_scaled1,
    out_scaled2,
    out_rows,
    out_cols1,
    out_cols2,
    hid_v,
    cot_v,
    perm_v,
    hid_t,
    grad,
    ship,
    ship_scale,
    land,
    land_scale,
    total,
    piece_out,
    piece_in,
    norm_out,
    norm_in,
    fresh,
    near,
    join,
    whole,
    col_out,
    col_in,
    row_out,
    row_in,
    local_sem,
    out_sem,
    ring_send,
    ring_recv,
    scale_send,
    scale_recv,
    plane_send,
    plane_recv,
    norm_send,
    norm_recv,
    near_send,
    near_recv,
    whole_send,
    whole_recv,
    col_send,
    col_recv,
    row_send,
    row_recv,
):
    xl = lax.axis_index("dp_0")
    z = lax.axis_index("dp_1")
    y = lax.axis_index("dp_2")
    xh = lax.axis_index("mp_0")
    core = lax.axis_index("mp_1")
    me = y + core * (z - y)
    other = z + core * (y - z)
    place = xl * 8 + other
    column = core * 8 + y
    sheet = (xl * 2 + xh) * 8 + z
    quad = xh * 2 + core

    def at(ring, across):
        return {"dp_1": across + core * (ring - across), "dp_2": ring + core * (across - ring)}

    def on_ring(c):
        return at(lax.rem(c + 16, 8), other)

    def in_plane(k):
        return {"dp_0": k // 8, **at(me, k % 8)}

    def in_column(k):
        return {"dp_2": k % 8, "mp_1": k // 8}

    def in_sheet(k):
        return {"dp_0": k // 16, "mp_0": (k // 8) % 2, "dp_1": k % 8}

    def in_quad(k):
        return {"mp_0": k // 2, "mp_1": k % 2}

    def remote(src, dst, send, recv, where):
        return pltpu.make_async_remote_copy(
            src_ref=src,
            dst_ref=dst,
            send_sem=send,
            recv_sem=recv,
            device_id=where,
            device_id_type=MESH,
        )

    def each_other(count, me, act):
        def body(i, carry):
            act(lax.rem(me + i, count))
            return carry

        first = count // 2 + 4 if count > 8 else count // 2
        lax.fori_loop(first, count, body, 0)
        lax.fori_loop(1, first, body, 0)

    def bytes_of(ref, sem):
        pltpu.make_async_copy(ref, ref, sem).wait()

    hid_copy = pltpu.make_async_copy(hid, hid_v, local_sem.at[PARTS])
    hid_copy.start()
    perm_copy = pltpu.make_async_copy(perm.at[core], perm_v, local_sem.at[PARTS + 1])
    perm_copy.start()
    cot_copies = []
    for q in range(PARTS):
        copy = pltpu.make_async_copy(
            cot.at[:, pl.ds(q * PART, PART)], cot_v.at[q], local_sem.at[q]
        )
        copy.start()
        cot_copies.append(copy)

    barrier = pltpu.get_barrier_semaphore()

    def greet(where):
        pl.semaphore_signal(barrier, inc=1, device_id=where, device_id_type=MESH)

    each_other(16, column, lambda k: greet(in_column(k)))
    each_other(32, sheet, lambda k: greet(in_sheet(k)))
    each_other(8, y, lambda k: greet({"dp_0": 1 - xl, "dp_2": k}))
    greet({"mp_0": 1 - xh, "mp_1": 1 - core})

    ring_copies = {}

    def send_ring(b, slot, distance, value):
        peak = jnp.maximum(jnp.max(jnp.abs(value), axis=0, keepdims=True), 1e-30)
        ship_scale[b, slot] = peak * (1.0 / TOP)
        coded = jnp.round(value * (TOP / peak))
        ship[b, slot] = coded.astype(I32).astype(I16)
        where = on_ring(me + distance)
        data = remote(
            ship.at[b, slot], land.at[b, slot], ring_send.at[b], ring_recv.at[b, slot], where
        )
        scale = remote(
            ship_scale.at[b, slot],
            land_scale.at[b, slot],
            scale_send.at[b],
            scale_recv.at[b, slot],
            where,
        )
        data.start()
        scale.start()
        ring_copies[b, slot] = (data, scale)

    def arrived(b, slot):
        data, scale = ring_copies[b, slot]
        data.wait_recv()
        scale.wait_recv()
        return land[b, slot].astype(I32).astype(F32) * land_scale[b, slot]

    def own(b, c):
        return grad[b, lax.rem(c + 16, 8)]

    def first_sends(b):
        way = long_way(b)
        send_ring(b, 6, 2 * way, own(b, me + 4))
        send_ring(b, 0, 1, own(b, me + 3))
        send_ring(b, 3, -1, own(b, me - 3))

    hid_copy.wait()
    perm_copy.wait()
    hid_t[...] = lax.dot_general(
        perm_v[...], hid_v[...], (((1,), (1,)), ((), ())), preferred_element_type=F32
    ).astype(BF16)
    for q in range(PARTS):
        cot_copies[q].wait()
        product = jnp.dot(hid_t[...], cot_v[q], preferred_element_type=F32)
        for b in (2 * q, 2 * q + 1):
            start = (b % 2) * WIDTH
            grad[b] = product[:, start : start + WIDTH].reshape(RING, CHUNK, WIDTH)
        if q == 0:
            pl.semaphore_wait(barrier, 15 + 31 + 7 + 1)
        for b in (2 * q, 2 * q + 1):
            first_sends(b)

    for b in range(BLOCKS):
        far = arrived(b, 6)
        ahead, behind = arrived(b, 0) + own(b, me + 2), arrived(b, 3) + own(b, me - 2)
        if long_way(b) > 0:
            ahead += far
        else:
            behind += far
        send_ring(b, 1, 1, ahead)
        send_ring(b, 4, -1, behind)
    for b in range(BLOCKS):
        send_ring(b, 2, 1, arrived(b, 1) + own(b, me + 1))
        send_ring(b, 5, -1, arrived(b, 4) + own(b, me - 1))
    for h in range(2):
        for i in range(4):
            b = 4 * h + i
            total[h, :, WIDTH * i : WIDTH * (i + 1)] = own(b, me) + arrived(b, 2) + arrived(b, 5)
        value = total[h]
        peak = jnp.maximum(jnp.max(jnp.abs(value), axis=0, keepdims=True), 1e-30)
        power = jnp.floor(jnp.log2(peak)) + 1.0
        total[h] = jnp.round(value * (TOP * jnp.exp2(-power)))
        for k in range(PLANE):
            piece = jnp.concatenate([total[h, OWN * k : OWN * k + OWN], power], axis=0)
            piece_out[h, k] = piece.astype(I32).astype(I16)
        piece_in[h, place] = piece_out[h, place]

        def send_piece(k, h=h):
            remote(
                piece_out.at[h, k],
                piece_in.at[h, place],
                plane_send.at[h],
                plane_recv.at[h],
                in_plane(k),
            ).start()

        each_other(PLANE, place, send_piece)

    def as_column(ref):
        at = lax.broadcasted_iota(I32, (OWN, 1), 0)
        return jnp.where(at == 0, ref[0], jnp.where(at == 1, ref[1], ref[2]))

    first_old = (
        (codes1[...].astype(F32) - 7.5) / 7.5 * jnp.minimum(as_column(rows1), cols1[...])
    )
    level = (codes2[...].astype(F32) + 1.0) / 16.0
    second_old = level * level * jnp.minimum(as_column(rows2), cols2[...])
    steps = jnp.full((1, 128), step[0].astype(F32))
    first_fix = (1.0 - jnp.exp(steps * np.float32(np.log(0.9))))[:, 0:1]
    second_fix = (1.0 - jnp.exp(steps * np.float32(np.log(0.95))))[:, 0:1]

    parts = {}
    for h in range(2):
        bytes_of(piece_in.at[h, pl.ds(0, PLANE - 1)], plane_recv.at[h])
        parts[h] = jnp.zeros((OWN, HALF), F32)
        for k in range(PLANE):
            piece = piece_in[h, k].astype(I32).astype(F32)
            unit = jnp.exp2(piece[OWN : OWN + 1]) * (1.0 / TOP)
            parts[h] = parts[h] + piece[0:OWN] * unit
    gradient = jnp.concatenate([parts[0], parts[1]], axis=1)

    square = jnp.sum(jnp.sum(gradient * gradient, axis=1, keepdims=True), axis=0, keepdims=True)
    square = jnp.broadcast_to(square, (1, 128))
    for phase, (count, mine, to) in enumerate(((16, column, in_column), (32, sheet, in_sheet))):
        norm_out[phase] = square
        norm_in[phase, mine] = square

        def send_norm(k, phase=phase, mine=mine, to=to):
            remote(
                norm_out.at[phase],
                norm_in.at[phase, mine],
                norm_send.at[phase],
                norm_recv.at[phase],
                to(k),
            ).start()

        each_other(count, mine, send_norm)
        bytes_of(norm_in.at[phase, pl.ds(0, count - 1)], norm_recv.at[phase])
        square = jnp.sum(norm_in[phase, 0:count], axis=0)

    entries = np.float32(3145728.0)
    limit = np.float32(0.01) * np.sqrt(entries)
    clipf = jnp.minimum(1.0, limit / (jnp.sqrt(square) + 1e-06))[:, 0:1]
    clipped = clipf * gradient
    first_new = 0.9 * first_old + 0.1 * clipped
    second_new = 0.95 * second_old + 0.05 * clipped * clipped
    ratio = first_new / first_fix / (jnp.sqrt(second_new / second_fix) + 1e-08)
    new_master = master[...] - 0.001 * (ratio + 0.1 * master[...])
    out_ratio[...] = ratio
    out_master[...] = new_master

    rounded = new_master.astype(BF16)
    for h in range(2):
        fresh[h] = rounded[:, h * HALF : (h + 1) * HALF]
        near[h, place] = rounded[:, h * HALF : (h + 1) * HALF]

        def send_near(k, h=h):
            remote(
                fresh.at[h], near.at[h, place], near_send.at[h], near_recv.at[h], in_plane(k)
            ).start()

        each_other(PLANE, place, send_near)

    first_abs = jnp.abs(first_new)
    row_out[0] = jnp.broadcast_to(jnp.max(first_abs, axis=1, keepdims=True), (OWN, 128))
    row_out[1] = jnp.broadcast_to(jnp.max(second_new, axis=1, keepdims=True), (OWN, 128))
    row_in[quad] = row_out[...]
    each_other(
        4,
        quad,
        lambda k: remote(row_out, row_in.at[quad], row_send, row_recv, in_quad(k)).start(),
    )
    tops = jnp.concatenate(
        [jnp.max(first_abs, axis=0, keepdims=True), jnp.max(second_new, axis=0, keepdims=True)],
        axis=0,
    )
    for k in range(PLANE):
        col_out[0, k] = tops[:, 128 * k : 128 * k + 128]
    col_in[0, place] = col_out[0, place]
    each_other(
        PLANE,
        place,
        lambda k: remote(
            col_out.at[0, k],
            col_in.at[0, place],
            col_send.at[0],
            col_recv.at[0],
            in_plane(k),
        ).start(),
    )

    whole_copies = {}

    def pass_on(b, slot, distance, c):
        at = lax.rem(c + 16, 8)
        copy = remote(
            whole.at[b, at],
            whole.at[b, at],
            whole_send.at[b],
            whole_recv.at[b, slot],
            on_ring(me + distance),
        )
        copy.start()
        whole_copies[b, slot] = copy

    for h in range(2):
        bytes_of(near.at[h, pl.ds(0, PLANE - 1)], near_recv.at[h])
        for k in range(PLANE):
            join[h, OWN * k : OWN * k + OWN] = near[h, k].astype(F32)
        for i in range(4):
            b = 4 * h + i
            whole[b, me] = join[h, :, WIDTH * i : WIDTH * (i + 1)].astype(BF16)
            pass_on(b, 0, 1, me)
            pass_on(b, 3, -1, me)

    bytes_of(col_in.at[0, pl.ds(0, PLANE - 1)], col_recv.at[0])
    best = jnp.max(col_in[0], axis=0)
    col_out[1, 0] = best
    col_in[1, me] = best
    each_other(
        RING,
        me,
        lambda c: remote(
            col_out.at[1, 0], col_in.at[1, me], col_send.at[1], col_recv.at[1], on_ring(c)
        ).start(),
    )

    def step_on(s):
        for b in range(BLOCKS):
            way = long_way(b)
            for first, direction in ((0, 1), (3, -1)):
                whole_copies[b, first + s - 1].wait_recv()
                if s == 2 and direction == way:
                    pass_on(b, 6, 2 * way, me - 2 * way)
                pass_on(b, first + s, direction, me - direction * s)

    step_on(1)
    step_on(2)

    bytes_of(col_in.at[1, pl.ds(0, 7)], col_recv.at[1])
    best = jnp.max(col_in[1, 0:8], axis=0)
    col_out[2, 0] = best
    col_in[2, place] = best
    each_other(
        PLANE,
        place,
        lambda k: remote(
            col_out.at[2, 0], col_in.at[2, place], col_send.at[2], col_recv.at[2], in_plane(k)
        ).start(),
    )
    bytes_of(row_in.at[pl.ds(0, 3)], row_recv)
    row_top = jnp.max(row_in[...], axis=0)
    out_rows[...] = row_top

    out_copies = []
    for b in range(BLOCKS):
        for slot in (2, 5, 6):
            whole_copies[b, slot].wait_recv()
        copy = pltpu.make_async_copy(whole.at[b], out_whole.at[b], out_sem.at[b])
        copy.start()
        out_copies.append(copy)

    bytes_of(col_in.at[2, pl.ds(0, PLANE - 1)], col_recv.at[2])
    for k in range(PLANE):
        out_cols1[:, 128 * k : 128 * k + 128] = col_in[2, k, 0:1]
        out_cols2[:, 128 * k : 128 * k + 128] = col_in[2, k, 1:2]
    out_scaled1[...] = first_new / (jnp.minimum(row_top[0, :, 0:1], out_cols1[...]) + 1e-08)
    out_scaled2[...] = second_new / (jnp.minimum(row_top[1, :, 0:1], out_cols2[...]) + 1e-08)

    for b in range(BLOCKS):
        bytes_of(ship.at[b], ring_send.at[b])
        bytes_of(ship_scale.at[b], scale_send.at[b])
        bytes_of(whole.at[b, pl.ds(0, 7)], whole_send.at[b])
    for h in range(2):
        bytes_of(piece_out.at[h, pl.ds(0, PLANE - 1)], plane_send.at[h])
        bytes_of(near.at[h, pl.ds(0, PLANE - 1)], near_send.at[h])
    for phase in range(2):
        bytes_of(norm_in.at[phase, pl.ds(0, 31 if phase else 15)], norm_send.at[phase])
    for phase in range(3):
        bytes_of(
            col_in.at[phase, pl.ds(0, 7 if phase == 1 else PLANE - 1)], col_send.at[phase]
        )
    bytes_of(row_in.at[pl.ds(0, 3)], row_send)
    for copy in out_copies:
        copy.wait()


def finish(
    whole,
    master,
    ratio,
    scaled1,
    scaled2,
    rows,
    cols1,
    cols2,
    back,
    out_master,
    out_ratio,
    out_params,
    out_scaled1,
    out_scaled2,
    out_rows1,
    out_cols1,
    out_rows2,
    out_cols2,
    whole_v,
    back_v,
    natural,
    own_v,
    col_v,
    row_v,
    in_sem,
    out_sem,
    own_sem,
):
    back_load = pltpu.make_async_copy(
        back.at[lax.axis_index("mp_1")], back_v, own_sem.at[7]
    )
    back_load.start()
    loads = [
        pltpu.make_async_copy(whole.at[b], whole_v.at[b], in_sem.at[b]) for b in range(BLOCKS)
    ]
    for copy in loads:
        copy.start()
    sources = (master, ratio, scaled1, scaled2)
    targets = (out_master, out_ratio, out_scaled1, out_scaled2)
    row_load = pltpu.make_async_copy(rows, row_v, own_sem.at[6])
    row_load.start()
    small = []
    for i in range(4):
        small.append((sources[i], own_v.at[i], targets[i], i))
    small.append((cols1, col_v.at[0], out_cols1, 4))
    small.append((cols2, col_v.at[1], out_cols2, 5))
    ins = [pltpu.make_async_copy(src, at, own_sem.at[i]) for src, at, _, i in small]
    for copy in ins:
        copy.start()
    outs = []
    back_load.wait()
    for q in range(PARTS):
        loads[2 * q].wait()
        loads[2 * q + 1].wait()
        part = jnp.concatenate(
            [whole_v[2 * q].reshape(ROWS, WIDTH), whole_v[2 * q + 1].reshape(ROWS, WIDTH)], axis=1
        )
        natural[q] = jnp.dot(back_v[...], part, preferred_element_type=F32).astype(BF16)
        copy = pltpu.make_async_copy(
            natural.at[q], out_params.at[:, pl.ds(q * PART, PART)], out_sem.at[q]
        )
        copy.start()
        outs.append(copy)
        if q == 0:
            row_load.wait()
            for j in range(OWN):
                out_rows1[j] = jnp.max(row_v[0, j : j + 1])
                out_rows2[j] = jnp.max(row_v[1, j : j + 1])
            for load, (_, at, target, i) in zip(ins, small, strict=True):
                load.wait()
                copy = pltpu.make_async_copy(at, target, own_sem.at[i])
                copy.start()
                outs.append(copy)
    for copy in outs:
        copy.wait()


def permutations():
    natural = np.arange(ROWS)
    by_y = natural.reshape(PLANE, RING, OWN).transpose(1, 0, 2).reshape(-1)
    by_z = natural.reshape(2, RING, RING, OWN).transpose(1, 0, 2, 3).reshape(-1)
    to_y = np.zeros((ROWS, ROWS), np.float32)
    to_y[natural, by_y] = 1.0
    to_z = np.zeros((ROWS, ROWS), np.float32)
    to_z[natural, by_z] = 1.0
    there = np.stack([to_y, to_z])
    return there, there.transpose(0, 2, 1)


def shards(
    hidden_input,
    output_cotangent,
    master_weights,
    first_codes,
    second_codes,
    first_rows,
    first_cols,
    second_rows,
    second_cols,
    step_count,
):
    own = jax.ShapeDtypeStruct((OWN, COLS), F32)
    row = jax.ShapeDtypeStruct((OWN,), F32)
    col = jax.ShapeDtypeStruct((1, COLS), F32)
    anywhere = pl.BlockSpec(memory_space=pl.ANY)
    hbm = pl.BlockSpec(memory_space=pltpu.HBM)
    vmem = pl.BlockSpec(memory_space=pltpu.VMEM)
    smem = pl.BlockSpec(memory_space=pltpu.SMEM)
    dma = pltpu.SemaphoreType.DMA
    perm, back = (jnp.asarray(p, BF16) for p in permutations())
    new_master, ratio, whole, scaled1, scaled2, rows, cols1, cols2 = pl.pallas_call(
        kernel,
        out_shape=(
            own,
            own,
            jax.ShapeDtypeStruct((BLOCKS, RING, CHUNK, WIDTH), BF16),
            own,
            own,
            jax.ShapeDtypeStruct((2, OWN, 128), F32),
            col,
            col,
        ),
        in_specs=[hbm, hbm, vmem, vmem, vmem, smem, vmem, smem, vmem, smem, hbm],
        out_specs=(vmem, vmem, anywhere, vmem, vmem, vmem, vmem, vmem),
        scratch_shapes=[
            pltpu.VMEM((TOKENS, ROWS), BF16),
            pltpu.VMEM((PARTS, TOKENS, PART), BF16),
            pltpu.VMEM((ROWS, ROWS), BF16),
            pltpu.VMEM((ROWS, TOKENS), BF16),
            pltpu.VMEM((BLOCKS, RING, CHUNK, WIDTH), F32),
            pltpu.VMEM((BLOCKS, 7, CHUNK, WIDTH), I16),
            pltpu.VMEM((BLOCKS, 7, 1, WIDTH), F32),
            pltpu.VMEM((BLOCKS, 7, CHUNK, WIDTH), I16),
            pltpu.VMEM((BLOCKS, 7, 1, WIDTH), F32),
            pltpu.VMEM((2, CHUNK, HALF), F32),
            pltpu.VMEM((2, PLANE, OWN + 1, HALF), I16),
            pltpu.VMEM((2, PLANE, OWN + 1, HALF), I16),
            pltpu.VMEM((2, 1, 128), F32),
            pltpu.VMEM((2, 32, 1, 128), F32),
            pltpu.VMEM((2, OWN, HALF), BF16),
            pltpu.VMEM((2, PLANE, OWN, HALF), BF16),
            pltpu.VMEM((2, CHUNK, HALF), F32),
            pltpu.VMEM((BLOCKS, RING, CHUNK, WIDTH), BF16),
            pltpu.VMEM((3, PLANE, 2, 128), F32),
            pltpu.VMEM((3, PLANE, 2, 128), F32),
            pltpu.VMEM((2, OWN, 128), F32),
            pltpu.VMEM((4, 2, OWN, 128), F32),
            dma((PARTS + 2,)),
            dma((BLOCKS,)),
            dma((BLOCKS,)),
            dma((BLOCKS, 7)),
            dma((BLOCKS,)),
            dma((BLOCKS, 7)),
            dma((2,)),
            dma((2,)),
            dma((3,)),
            dma((3,)),
            dma((2,)),
            dma((2,)),
            dma((BLOCKS,)),
            dma((BLOCKS, 7)),
            dma((3,)),
            dma((3,)),
            dma,
            dma,
        ],
        compiler_params=pltpu.CompilerParams(
            collective_id=0, has_side_effects=True, vmem_limit_bytes=60 * 1024 * 1024
        ),
    )(
        hidden_input,
        output_cotangent,
        master_weights,
        first_codes,
        second_codes,
        first_rows,
        first_cols.reshape(1, -1),
        second_rows,
        second_cols.reshape(1, -1),
        step_count.reshape(1),
        perm,
    )
    outs = pl.pallas_call(
        finish,
        out_shape=(
            own,
            own,
            jax.ShapeDtypeStruct((ROWS, COLS), BF16),
            own,
            own,
            row,
            col,
            row,
            col,
        ),
        in_specs=[anywhere] * 8 + [hbm],
        out_specs=(hbm, hbm, hbm, hbm, hbm, smem, hbm, smem, hbm),
        scratch_shapes=[
            pltpu.VMEM((BLOCKS, RING, CHUNK, WIDTH), BF16),
            pltpu.VMEM((ROWS, ROWS), BF16),
            pltpu.VMEM((PARTS, ROWS, PART), BF16),
            pltpu.VMEM((4, OWN, COLS), F32),
            pltpu.VMEM((2, 1, COLS), F32),
            pltpu.VMEM((2, OWN, 128), F32),
            dma((BLOCKS,)),
            dma((BLOCKS,)),
            dma((8,)),
        ],
        compiler_params=pltpu.CompilerParams(vmem_limit_bytes=60 * 1024 * 1024),
    )(whole, new_master, ratio, scaled1, scaled2, rows, cols1, cols2, back)
    outs = list(outs)
    outs[6] = outs[6].reshape(-1)
    outs[8] = outs[8].reshape(-1)
    return tuple(outs)


def solution(mesh):
    finer = Mesh(mesh.devices.reshape(2, 8, 8, 2, 2), ("dp_0", "dp_1", "dp_2", "mp_0", "mp_1"))
    in_specs = (
        P(DP, None),
        P(DP, MP),
        P(DP, MP),
        P(DP, MP),
        P(DP, MP),
        P(DP),
        P(MP),
        P(DP),
        P(MP),
        P(),
    )
    out_specs = (
        P(DP, MP),
        P(DP, MP),
        P(None, MP),
        P(DP, MP),
        P(DP, MP),
        P(DP),
        P(MP),
        P(DP),
        P(MP),
    )
    return jax.shard_map(
        shards, mesh=finer, in_specs=in_specs, out_specs=out_specs, check_vma=False
    )
```

```python
import jax
import jax.numpy as jnp
import numpy as np
from jax import lax
from jax.experimental import pallas as pl
from jax.experimental.pallas import tpu as pltpu
from jax.sharding import Mesh
from jax.sharding import PartitionSpec as P

DP = ("dp_0", "dp_1", "dp_2")
MP = ("mp_0", "mp_1")
MESH = pl.DeviceIdType.MESH
F32, BF16, I16, I32 = jnp.float32, jnp.bfloat16, jnp.int16, jnp.int32

RING = 8
PLANE = 16
OWN = 3
CHUNK = PLANE * OWN
ROWS = RING * CHUNK
COLS = 2048
WIDTH = 512
BLOCKS = 4
HALF = 1024
TOKENS = 1024
TOP = 32767.0
NEED = (4, 3, -3, 2, -2, 1, -1, 0)
FAR = 3


def long_way(b):
    return 1 if b % 2 else -1


def steps_of(b):
    return 4 if b < BLOCKS // 2 else 3


def kernel(
    hid,
    cot,
    master,
    codes1,
    codes2,
    rows1,
    cols1,
    rows2,
    cols2,
    step,
    perm,
    back,
    out_master,
    out_ratio,
    out_natural,
    out_scaled1,
    out_scaled2,
    out_rows,
    out_cols1,
    out_cols2,
    master_v,
    codes_v,
    cols_v,
    rows1_s,
    rows2_s,
    step_s,
    result_v,
    row_result,
    col_result,
    hid_v,
    cot_v,
    perm_v,
    back_v,
    hid_t,
    grad,
    ship,
    ship_scale,
    land,
    land_scale,
    total,
    piece_out,
    piece_in,
    norm_out,
    norm_in,
    fresh,
    near,
    join,
    whole,
    natural,
    col_out,
    col_in,
    row_out,
    row_in,
    news,
    input_sem,
    result_sem,
    local_sem,
    perm_sem,
    out_sem,
    ring_send,
    ring_recv,
    scale_send,
    scale_recv,
    plane_send,
    plane_recv,
    norm_send,
    norm_recv,
    near_send,
    near_recv,
    whole_send,
    whole_recv,
    col_send,
    col_recv,
    row_send,
    row_recv,
):
    xl = lax.axis_index("dp_0")
    z = lax.axis_index("dp_1")
    y = lax.axis_index("dp_2")
    xh = lax.axis_index("mp_0")
    core = lax.axis_index("mp_1")
    me = y + core * (z - y)
    other = z + core * (y - z)
    place = xl * 8 + other
    column = core * 8 + y
    sheet = (xl * 2 + xh) * 8 + z
    quad = xh * 2 + core

    def at(ring, across):
        return {"dp_1": across + core * (ring - across), "dp_2": ring + core * (across - ring)}

    def on_ring(c):
        return at(lax.rem(c + 16, 8), other)

    def in_plane(k):
        return {"dp_0": k // 8, **at(me, k % 8)}

    def in_column(k):
        return {"dp_2": k % 8, "mp_1": k // 8}

    def in_sheet(k):
        return {"dp_0": k // 16, "mp_0": (k // 8) % 2, "dp_1": k % 8}

    def in_quad(k):
        return {"mp_0": k // 2, "mp_1": k % 2}

    def remote(src, dst, send, recv, where):
        return pltpu.make_async_remote_copy(
            src_ref=src,
            dst_ref=dst,
            send_sem=send,
            recv_sem=recv,
            device_id=where,
            device_id_type=MESH,
        )

    def each_other(count, me, act):
        def body(i, carry):
            act(lax.rem(me + i, count))
            return carry

        first = count // 2 + 4 if count > 8 else count // 2
        lax.fori_loop(first, count, body, 0, unroll=4)
        lax.fori_loop(1, first, body, 0, unroll=4)

    def bytes_of(ref, sem):
        pltpu.make_async_copy(ref, ref, sem).wait()

    hid_copy = pltpu.make_async_copy(hid, hid_v, local_sem.at[BLOCKS])
    hid_copy.start()
    perm_copy = pltpu.make_async_copy(perm.at[core], perm_v, perm_sem)
    perm_copy.start()
    cot_copies = []
    for q in range(BLOCKS):
        copy = pltpu.make_async_copy(
            cot.at[:, pl.ds(q * WIDTH, WIDTH)], cot_v.at[q], local_sem.at[q]
        )
        cot_copies.append(copy)
    cot_copies[0].start()
    back_copy = pltpu.make_async_copy(back.at[core], back_v, local_sem.at[BLOCKS + 1])
    inputs = (
        (master, master_v),
        (codes1, codes_v.at[0]),
        (codes2, codes_v.at[1]),
        (cols1, cols_v.at[0]),
        (cols2, cols_v.at[1]),
        (rows1, rows1_s),
        (rows2, rows2_s),
        (step, step_s),
    )
    input_copies = [
        pltpu.make_async_copy(src, dst, input_sem.at[i]) for i, (src, dst) in enumerate(inputs)
    ]

    barrier = pltpu.get_barrier_semaphore()

    def greet(where):
        pl.semaphore_signal(barrier, inc=1, device_id=where, device_id_type=MESH)

    for distance in (2, -2, 1, -1):
        greet(on_ring(me + distance))
    for distance in (1, -1):
        across = at(me, lax.rem(other + distance + 8, 8))
        greet(across)
        greet({"dp_0": 1 - xl, **across})
    greet({"dp_0": 1 - xl})
    each_other(4, quad, lambda k: greet(in_quad(k)))

    def tell(i):
        for distance in (1, -1):
            pl.semaphore_signal(
                news.at[i],
                inc=1,
                device_id=at(me, lax.rem(other + distance + 8, 8)),
                device_id_type=MESH,
            )

    def hear(i):
        pl.semaphore_wait(news.at[i], 2)

    ring_copies = {}

    def send_ring(b, slot, distance, value):
        peak = jnp.maximum(jnp.max(jnp.abs(value), axis=0, keepdims=True), 1e-30)
        ship_scale[b, slot] = peak * (1.0 / TOP)
        coded = jnp.round(value * (TOP / peak))
        ship[b, slot] = coded.astype(I32).astype(I16)
        where = on_ring(me + distance)
        data = remote(
            ship.at[b, slot], land.at[b, slot], ring_send.at[b], ring_recv.at[b, slot], where
        )
        scale = remote(
            ship_scale.at[b, slot],
            land_scale.at[b, slot],
            scale_send.at[b],
            scale_recv.at[b, slot],
            where,
        )
        data.start()
        scale.start()
        ring_copies[b, slot] = (data, scale)

    def arrived(b, slot):
        data, scale = ring_copies[b, slot]
        data.wait_recv()
        scale.wait_recv()
        return land[b, slot].astype(I32).astype(F32) * land_scale[b, slot]

    def own(b, distance):
        return grad[b, NEED.index(distance)]

    def slots(b):
        return (0, 3) if long_way(b) > 0 else (3, 0)

    def first_sends(b):
        way = long_way(b)
        long, short = slots(b)
        send_ring(b, 6, way if steps_of(b) == 4 else 2 * way, own(b, 4))
        if steps_of(b) == 3:
            send_ring(b, long, way, own(b, 3 * way))
        send_ring(b, short, -way, own(b, -3 * way))

    hid_copy.wait()
    perm_copy.wait()
    for copy in (*cot_copies[1:], *input_copies, back_copy):
        copy.start()
    hid_t[...] = lax.dot_general(
        perm_v[...],
        hid_v[...],
        (((1,), (1,)), ((), ())),
        preferred_element_type=F32,
    ).astype(BF16)

    def multiply(b, first, last):
        lhs = jnp.concatenate(
            [
                hid_t[pl.ds(pl.multiple_of(lax.rem(me + d + 8, 8) * CHUNK, CHUNK), CHUNK)]
                for d in NEED[first:last]
            ],
            axis=0,
        )
        product = jnp.dot(lhs, cot_v[b], preferred_element_type=F32)
        grad[b, first:last] = product.reshape(last - first, CHUNK, WIDTH)

    for b in range(BLOCKS):
        cot_copies[b].wait()
        multiply(b, 0, FAR)
        if b == 0:
            pl.semaphore_wait(barrier, 4 + 4 + 1 + 3)
            tell(0)
        first_sends(b)
    for b in range(BLOCKS):
        multiply(b, FAR, RING)
    hear(0)
    tell(1)

    for b in range(BLOCKS):
        way = long_way(b)
        long, short = slots(b)
        far = arrived(b, 6)
        if steps_of(b) == 4:
            send_ring(b, long, way, far + own(b, 3 * way))
        else:
            send_ring(b, long + 1, way, far + arrived(b, long) + own(b, 2 * way))
        send_ring(b, short + 1, -way, arrived(b, short) + own(b, -2 * way))
    hear(1)
    tell(2)
    for b in range(BLOCKS):
        way = long_way(b)
        long, short = slots(b)
        if steps_of(b) == 4:
            send_ring(b, long + 1, way, arrived(b, long) + own(b, 2 * way))
        else:
            send_ring(b, long + 2, way, arrived(b, long + 1) + own(b, way))
        send_ring(b, short + 2, -way, arrived(b, short + 1) + own(b, -way))
    hear(2)
    for b in range(BLOCKS // 2):
        way = long_way(b)
        long, _ = slots(b)
        send_ring(b, long + 2, way, arrived(b, long + 1) + own(b, way))
    for h in (1, 0):
        for i in range(2):
            b = 2 * h + i
            total[h, :, WIDTH * i : WIDTH * (i + 1)] = own(b, 0) + arrived(b, 2) + arrived(b, 5)
        value = total[h]
        peak = jnp.maximum(jnp.max(jnp.abs(value), axis=0, keepdims=True), 1e-30)
        power = jnp.floor(jnp.log2(peak)) + 1.0
        total[h] = jnp.round(value * (TOP * jnp.exp2(-power)))
        for k in range(PLANE):
            piece = jnp.concatenate([total[h, OWN * k : OWN * k + OWN], power], axis=0)
            piece_out[h, k] = piece.astype(I32).astype(I16)
        piece_in[h, place] = piece_out[h, place]

        def send_piece(k, h=h):
            remote(
                piece_out.at[h, k],
                piece_in.at[h, place],
                plane_send.at[h],
                plane_recv.at[h],
                in_plane(k),
            ).start()

        each_other(PLANE, place, send_piece)

    def as_column(ref):
        at = lax.broadcasted_iota(I32, (OWN, 1), 0)
        return jnp.where(at == 0, ref[0], jnp.where(at == 1, ref[1], ref[2]))

    for copy in input_copies:
        copy.wait()
    first_old = (
        (codes_v[0].astype(F32) - 7.5) / 7.5 * jnp.minimum(as_column(rows1_s), cols_v[0])
    )
    level = (codes_v[1].astype(F32) + 1.0) / 16.0
    second_old = level * level * jnp.minimum(as_column(rows2_s), cols_v[1])
    steps = jnp.full((1, 128), step_s[0].astype(F32))
    first_fix = (1.0 - jnp.exp(steps * np.float32(np.log(0.9))))[:, 0:1]
    second_fix = (1.0 - jnp.exp(steps * np.float32(np.log(0.95))))[:, 0:1]

    parts = {}
    for h in (1, 0):
        bytes_of(piece_in.at[h, pl.ds(0, PLANE - 1)], plane_recv.at[h])
        parts[h] = jnp.zeros((OWN, HALF), F32)
        for k in range(PLANE):
            piece = piece_in[h, k].astype(I32).astype(F32)
            unit = jnp.exp2(piece[OWN : OWN + 1]) * (1.0 / TOP)
            parts[h] = parts[h] + piece[0:OWN] * unit
    gradient = jnp.concatenate([parts[0], parts[1]], axis=1)

    square = jnp.sum(jnp.sum(gradient * gradient, axis=1, keepdims=True), axis=0, keepdims=True)
    square = jnp.broadcast_to(square, (1, 128))
    for phase, (count, mine, to) in enumerate(((16, column, in_column), (32, sheet, in_sheet))):
        norm_out[phase] = square
        norm_in[phase, mine] = square

        def send_norm(k, phase=phase, mine=mine, to=to):
            remote(
                norm_out.at[phase],
                norm_in.at[phase, mine],
                norm_send.at[phase],
                norm_recv.at[phase],
                to(k),
            ).start()

        each_other(count, mine, send_norm)
        bytes_of(norm_in.at[phase, pl.ds(0, count - 1)], norm_recv.at[phase])
        square = jnp.sum(norm_in[phase, 0:count], axis=0)

    entries = np.float32(3145728.0)
    limit = np.float32(0.01) * np.sqrt(entries)
    clipf = jnp.minimum(1.0, limit / (jnp.sqrt(square) + 1e-06))[:, 0:1]
    clipped = clipf * gradient
    first_new = 0.9 * first_old + 0.1 * clipped
    second_new = 0.95 * second_old + 0.05 * clipped * clipped
    ratio = first_new / first_fix / (jnp.sqrt(second_new / second_fix) + 1e-08)
    new_master = master_v[...] - 0.001 * (ratio + 0.1 * master_v[...])

    rounded = new_master.astype(BF16)
    fresh[...] = rounded
    near[place] = rounded
    each_other(
        PLANE,
        place,
        lambda k: remote(fresh, near.at[place], near_send, near_recv, in_plane(k)).start(),
    )

    results = (
        (result_v.at[0], out_master),
        (result_v.at[1], out_ratio),
        (result_v.at[2], out_scaled1),
        (result_v.at[3], out_scaled2),
        (row_result, out_rows),
        (col_result.at[0], out_cols1),
        (col_result.at[1], out_cols2),
    )
    result_copies = [
        pltpu.make_async_copy(src, dst, result_sem.at[i]) for i, (src, dst) in enumerate(results)
    ]
    result_v[0] = new_master
    result_v[1] = ratio
    result_copies[0].start()
    result_copies[1].start()

    first_abs = jnp.abs(first_new)
    row_out[0] = jnp.broadcast_to(jnp.max(first_abs, axis=1, keepdims=True), (OWN, 128))
    row_out[1] = jnp.broadcast_to(jnp.max(second_new, axis=1, keepdims=True), (OWN, 128))
    row_in[quad] = row_out[...]
    each_other(
        4,
        quad,
        lambda k: remote(row_out, row_in.at[quad], row_send, row_recv, in_quad(k)).start(),
    )
    tops = jnp.concatenate(
        [jnp.max(first_abs, axis=0, keepdims=True), jnp.max(second_new, axis=0, keepdims=True)],
        axis=0,
    )
    for k in range(PLANE):
        col_out[0, k] = tops[:, 128 * k : 128 * k + 128]
    col_in[0, place] = col_out[0, place]
    each_other(
        PLANE,
        place,
        lambda k: remote(
            col_out.at[0, k],
            col_in.at[0, place],
            col_send.at[0],
            col_recv.at[0],
            in_plane(k),
        ).start(),
    )

    whole_copies = {}

    def pass_on(b, slot, distance, c):
        at = lax.rem(c + 16, 8)
        copy = remote(
            whole.at[b, at],
            whole.at[b, at],
            whole_send.at[b],
            whole_recv.at[b, slot],
            on_ring(me + distance),
        )
        copy.start()
        whole_copies[b, slot] = copy

    bytes_of(near.at[pl.ds(0, PLANE - 1)], near_recv)
    for b in range(BLOCKS):
        for k in range(PLANE):
            join[b, OWN * k : OWN * k + OWN] = near[k, :, WIDTH * b : WIDTH * (b + 1)].astype(F32)
        whole[b, me] = join[b].astype(BF16)
        pass_on(b, 0, 1, me)
        pass_on(b, 3, -1, me)

    bytes_of(col_in.at[0, pl.ds(0, PLANE - 1)], col_recv.at[0])
    best = jnp.max(col_in[0], axis=0)
    col_out[1, 0] = best
    col_in[1, me] = best
    each_other(
        RING,
        me,
        lambda c: remote(
            col_out.at[1, 0], col_in.at[1, me], col_send.at[1], col_recv.at[1], on_ring(c)
        ).start(),
    )

    def step_on(s):
        for b in range(BLOCKS):
            way = long_way(b)
            for first, direction in ((0, 1), (3, -1)):
                whole_copies[b, first + s - 1].wait_recv()
                if s == 2 and direction == way and steps_of(b) == 3:
                    pass_on(b, 6, 2 * way, me - 2 * way)
                pass_on(b, first + s, direction, me - direction * s)

    step_on(1)
    step_on(2)

    bytes_of(col_in.at[1, pl.ds(0, 7)], col_recv.at[1])
    best = jnp.max(col_in[1, 0:8], axis=0)
    col_out[2, 0] = best
    col_in[2, place] = best
    each_other(
        PLANE,
        place,
        lambda k: remote(
            col_out.at[2, 0], col_in.at[2, place], col_send.at[2], col_recv.at[2], in_plane(k)
        ).start(),
    )
    bytes_of(row_in.at[pl.ds(0, 3)], row_recv)
    row_top = jnp.max(row_in[...], axis=0)
    row_result[...] = row_top
    result_copies[4].start()

    for b in range(BLOCKS // 2):
        way = long_way(b)
        long, _ = slots(b)
        whole_copies[b, long + 2].wait_recv()
        pass_on(b, 6, way, me - 3 * way)

    back_copy.wait()
    out_copies = []
    for b in (2, 3, 0, 1):
        for slot in (2, 5, 6):
            if steps_of(b) == 3 or slot != slots(b)[0] + 2:
                whole_copies[b, slot].wait_recv()
        block = whole[b].reshape(ROWS, WIDTH)
        natural[b] = jnp.dot(back_v[...], block, preferred_element_type=F32).astype(BF16)
        copy = pltpu.make_async_copy(
            natural.at[b], out_natural.at[:, pl.ds(b * WIDTH, WIDTH)], out_sem.at[b]
        )
        copy.start()
        out_copies.append(copy)

    bytes_of(col_in.at[2, pl.ds(0, PLANE - 1)], col_recv.at[2])
    for k in range(PLANE):
        col_result[0, :, 128 * k : 128 * k + 128] = col_in[2, k, 0:1]
        col_result[1, :, 128 * k : 128 * k + 128] = col_in[2, k, 1:2]
    result_v[2] = first_new / (jnp.minimum(row_top[0, :, 0:1], col_result[0]) + 1e-08)
    result_v[3] = second_new / (jnp.minimum(row_top[1, :, 0:1], col_result[1]) + 1e-08)
    for i in (2, 3, 5, 6):
        result_copies[i].start()

    for b in range(BLOCKS):
        bytes_of(ship.at[b], ring_send.at[b])
        bytes_of(ship_scale.at[b], scale_send.at[b])
        bytes_of(whole.at[b, pl.ds(0, 7)], whole_send.at[b])
    for h in range(2):
        bytes_of(piece_out.at[h, pl.ds(0, PLANE - 1)], plane_send.at[h])
    for phase in range(2):
        bytes_of(norm_in.at[phase, pl.ds(0, 31 if phase else 15)], norm_send.at[phase])
    for phase in range(3):
        bytes_of(
            col_in.at[phase, pl.ds(0, 7 if phase == 1 else PLANE - 1)], col_send.at[phase]
        )
    bytes_of(near.at[pl.ds(0, PLANE - 1)], near_send)
    bytes_of(row_in.at[pl.ds(0, 3)], row_send)
    for copy in (*out_copies, *result_copies):
        copy.wait()


def finish(
    natural,
    master,
    ratio,
    scaled1,
    scaled2,
    rows,
    cols1,
    cols2,
    out_master,
    out_ratio,
    out_params,
    out_scaled1,
    out_scaled2,
    out_rows1,
    out_cols1,
    out_rows2,
    out_cols2,
    natural_v,
    own_v,
    col_v,
    row_v,
    row1_s,
    row2_s,
    big_sem,
    small_sem,
):
    moves = []
    for i in range(RING):
        at = pl.ds(i * CHUNK, CHUNK)
        moves.append((natural.at[at], natural_v.at[at], out_params.at[at], big_sem.at[i]))
    sources = (master, ratio, scaled1, scaled2)
    targets = (out_master, out_ratio, out_scaled1, out_scaled2)
    for i in range(4):
        moves.append((sources[i], own_v.at[i], targets[i], small_sem.at[i]))
    moves.append((cols1, col_v.at[0], out_cols1, small_sem.at[4]))
    moves.append((cols2, col_v.at[1], out_cols2, small_sem.at[5]))
    row_load = pltpu.make_async_copy(rows, row_v, small_sem.at[6])
    row_load.start()
    ins = [pltpu.make_async_copy(src, at, sem) for src, at, _, sem in moves]
    for copy in ins:
        copy.start()
    outs = []
    for load, (_, at, target, sem) in zip(ins, moves, strict=True):
        load.wait()
        copy = pltpu.make_async_copy(at, target, sem)
        copy.start()
        outs.append(copy)
    row_load.wait()
    for j in range(OWN):
        row1_s[j] = jnp.max(row_v[0, j : j + 1])
        row2_s[j] = jnp.max(row_v[1, j : j + 1])
    for i, (src, dst) in enumerate(((row1_s, out_rows1), (row2_s, out_rows2))):
        copy = pltpu.make_async_copy(src, dst, small_sem.at[6 + i])
        copy.start()
        outs.append(copy)
    for copy in outs:
        copy.wait()


def permutations():
    natural = np.arange(ROWS)
    by_y = natural.reshape(PLANE, RING, OWN).transpose(1, 0, 2).reshape(-1)
    by_z = natural.reshape(2, RING, RING, OWN).transpose(1, 0, 2, 3).reshape(-1)
    to_y = np.zeros((ROWS, ROWS), np.float32)
    to_y[natural, by_y] = 1.0
    to_z = np.zeros((ROWS, ROWS), np.float32)
    to_z[natural, by_z] = 1.0
    there = np.stack([to_y, to_z])
    return there, there.transpose(0, 2, 1)


def shards(
    hidden_input,
    output_cotangent,
    master_weights,
    first_codes,
    second_codes,
    first_rows,
    first_cols,
    second_rows,
    second_cols,
    step_count,
):
    own = jax.ShapeDtypeStruct((OWN, COLS), F32)
    row = jax.ShapeDtypeStruct((OWN,), F32)
    col = jax.ShapeDtypeStruct((1, COLS), F32)
    anywhere = pl.BlockSpec(memory_space=pl.ANY)
    hbm = pl.BlockSpec(memory_space=pltpu.HBM)
    dma = pltpu.SemaphoreType.DMA
    perm, back = (jnp.asarray(p, BF16) for p in permutations())
    new_master, ratio, natural, scaled1, scaled2, rows, cols1, cols2 = pl.pallas_call(
        kernel,
        out_shape=(
            own,
            own,
            jax.ShapeDtypeStruct((ROWS, COLS), BF16),
            own,
            own,
            jax.ShapeDtypeStruct((2, OWN, 128), F32),
            col,
            col,
        ),
        in_specs=[hbm] * 12,
        out_specs=(hbm,) * 8,
        scratch_shapes=[
            pltpu.VMEM((OWN, COLS), F32),
            pltpu.VMEM((2, OWN, COLS), I32),
            pltpu.VMEM((2, 1, COLS), F32),
            pltpu.SMEM((OWN,), F32),
            pltpu.SMEM((OWN,), F32),
            pltpu.SMEM((1,), I32),
            pltpu.VMEM((4, OWN, COLS), F32),
            pltpu.VMEM((2, OWN, 128), F32),
            pltpu.VMEM((2, 1, COLS), F32),
            pltpu.VMEM((TOKENS, ROWS), BF16),
            pltpu.VMEM((BLOCKS, TOKENS, WIDTH), BF16),
            pltpu.VMEM((ROWS, ROWS), BF16),
            pltpu.VMEM((ROWS, ROWS), BF16),
            pltpu.VMEM((ROWS, TOKENS), BF16),
            pltpu.VMEM((BLOCKS, RING, CHUNK, WIDTH), F32),
            pltpu.VMEM((BLOCKS, 7, CHUNK, WIDTH), I16),
            pltpu.VMEM((BLOCKS, 7, 1, WIDTH), F32),
            pltpu.VMEM((BLOCKS, 7, CHUNK, WIDTH), I16),
            pltpu.VMEM((BLOCKS, 7, 1, WIDTH), F32),
            pltpu.VMEM((2, CHUNK, HALF), F32),
            pltpu.VMEM((2, PLANE, OWN + 1, HALF), I16),
            pltpu.VMEM((2, PLANE, OWN + 1, HALF), I16),
            pltpu.VMEM((2, 1, 128), F32),
            pltpu.VMEM((2, 32, 1, 128), F32),
            pltpu.VMEM((OWN, COLS), BF16),
            pltpu.VMEM((PLANE, OWN, COLS), BF16),
            pltpu.VMEM((BLOCKS, CHUNK, WIDTH), F32),
            pltpu.VMEM((BLOCKS, RING, CHUNK, WIDTH), BF16),
            pltpu.VMEM((BLOCKS, ROWS, WIDTH), BF16),
            pltpu.VMEM((3, PLANE, 2, 128), F32),
            pltpu.VMEM((3, PLANE, 2, 128), F32),
            pltpu.VMEM((2, OWN, 128), F32),
            pltpu.VMEM((4, 2, OWN, 128), F32),
            pltpu.SemaphoreType.REGULAR((3,)),
            dma((8,)),
            dma((7,)),
            dma((BLOCKS + 2,)),
            dma,
            dma((BLOCKS,)),
            dma((BLOCKS,)),
            dma((BLOCKS, 7)),
            dma((BLOCKS,)),
            dma((BLOCKS, 7)),
            dma((2,)),
            dma((2,)),
            dma((2,)),
            dma((2,)),
            dma,
            dma,
            dma((BLOCKS,)),
            dma((BLOCKS, 7)),
            dma((3,)),
            dma((3,)),
            dma,
            dma,
        ],
        compiler_params=pltpu.CompilerParams(
            collective_id=0, has_side_effects=True, vmem_limit_bytes=60 * 1024 * 1024
        ),
    )(
        hidden_input,
        output_cotangent,
        master_weights,
        first_codes,
        second_codes,
        first_rows,
        first_cols.reshape(1, -1),
        second_rows,
        second_cols.reshape(1, -1),
        step_count.reshape(1),
        perm,
        back,
    )
    outs = pl.pallas_call(
        finish,
        out_shape=(
            own,
            own,
            jax.ShapeDtypeStruct((ROWS, COLS), BF16),
            own,
            own,
            row,
            col,
            row,
            col,
        ),
        in_specs=[anywhere] * 8,
        out_specs=(hbm,) * 9,
        scratch_shapes=[
            pltpu.VMEM((ROWS, COLS), BF16),
            pltpu.VMEM((4, OWN, COLS), F32),
            pltpu.VMEM((2, 1, COLS), F32),
            pltpu.VMEM((2, OWN, 128), F32),
            pltpu.SMEM((OWN,), F32),
            pltpu.SMEM((OWN,), F32),
            dma((RING,)),
            dma((8,)),
        ],
        compiler_params=pltpu.CompilerParams(vmem_limit_bytes=60 * 1024 * 1024),
    )(natural, new_master, ratio, scaled1, scaled2, rows, cols1, cols2)
    outs = list(outs)
    outs[6] = outs[6].reshape(-1)
    outs[8] = outs[8].reshape(-1)
    return tuple(outs)


def solution(mesh):
    finer = Mesh(mesh.devices.reshape(2, 8, 8, 2, 2), ("dp_0", "dp_1", "dp_2", "mp_0", "mp_1"))
    in_specs = (
        P(DP, None),
        P(DP, MP),
        P(DP, MP),
        P(DP, MP),
        P(DP, MP),
        P(DP),
        P(MP),
        P(DP),
        P(MP),
        P(),
    )
    out_specs = (
        P(DP, MP),
        P(DP, MP),
        P(None, MP),
        P(DP, MP),
        P(DP, MP),
        P(DP),
        P(MP),
        P(DP),
        P(MP),
    )
    return jax.shard_map(
        shards, mesh=finer, in_specs=in_specs, out_specs=out_specs, check_vma=False
    )
```

```python
import jax
import jax.numpy as jnp
import numpy as np
from jax import lax
from jax.experimental import pallas as pl
from jax.experimental.pallas import tpu as pltpu
from jax.sharding import Mesh
from jax.sharding import PartitionSpec as P

DP = ("dp_0", "dp_1", "dp_2")
MP = ("mp_0", "mp_1")
MESH = pl.DeviceIdType.MESH
F32, BF16, I16, I32 = jnp.float32, jnp.bfloat16, jnp.int16, jnp.int32

RING = 8
PLANE = 16
OWN = 3
CHUNK = PLANE * OWN
ROWS = RING * CHUNK
COLS = 2048
WIDTH = 512
BLOCKS = 4
HALF = 1024
TOKENS = 1024
TOP = 32767.0
NEED = (4, 3, -3, 2, -2, 1, -1, 0)
FAR = 3


def long_way(b):
    return 1 if b % 2 else -1


def steps_of(b):
    return 4 if b < BLOCKS // 2 else 3


def kernel(
    hid,
    cot,
    master,
    codes1,
    codes2,
    rows1,
    cols1,
    rows2,
    cols2,
    step,
    perm,
    back,
    out_master,
    out_ratio,
    out_natural,
    out_scaled1,
    out_scaled2,
    out_rows,
    out_cols1,
    out_cols2,
    master_v,
    codes_v,
    cols_v,
    rows1_s,
    rows2_s,
    step_s,
    result_v,
    row_result,
    col_result,
    hid_v,
    cot_v,
    perm_v,
    back_v,
    hid_t,
    grad,
    ship,
    ship_scale,
    land,
    land_scale,
    total,
    piece_out,
    piece_in,
    norm_out,
    norm_in,
    fresh,
    near,
    join,
    whole,
    natural,
    col_out,
    col_in,
    row_out,
    row_in,
    news,
    input_sem,
    local_sem,
    perm_sem,
    ring_send,
    ring_recv,
    scale_send,
    scale_recv,
    plane_send,
    plane_recv,
    norm_send,
    norm_recv,
    near_send,
    near_recv,
    whole_send,
    col_send,
    col_recv,
    row_send,
    row_recv,
):
    xl = lax.axis_index("dp_0")
    z = lax.axis_index("dp_1")
    y = lax.axis_index("dp_2")
    xh = lax.axis_index("mp_0")
    core = lax.axis_index("mp_1")
    me = z + core * (y - z)
    other = y + core * (z - y)
    place = xl * 8 + other
    column = core * 8 + y
    sheet = (xl * 2 + xh) * 8 + z
    quad = xh * 2 + core

    def at(ring, across):
        return {"dp_1": ring + core * (across - ring), "dp_2": across + core * (ring - across)}

    def on_ring(c):
        return at(lax.rem(c + 16, 8), other)

    def in_plane(k):
        return {"dp_0": k // 8, **at(me, k % 8)}

    def in_column(k):
        return {"dp_2": k % 8, "mp_1": k // 8}

    def in_sheet(k):
        return {"dp_0": k // 16, "mp_0": (k // 8) % 2, "dp_1": k % 8}

    def in_quad(k):
        return {"mp_0": k // 2, "mp_1": k % 2}

    def remote(src, dst, send, recv, where):
        return pltpu.make_async_remote_copy(
            src_ref=src,
            dst_ref=dst,
            send_sem=send,
            recv_sem=recv,
            device_id=where,
            device_id_type=MESH,
        )

    def each_other(count, me, act):
        def body(i, carry):
            act(lax.rem(me + i, count))
            return carry

        first = count // 2 + 4 if count > 8 else count // 2
        lax.fori_loop(first, count, body, 0, unroll=4)
        lax.fori_loop(1, first, body, 0, unroll=4)

    def bytes_of(ref, sem):
        pltpu.make_async_copy(ref, ref, sem).wait()

    hid_copy = pltpu.make_async_copy(hid, hid_v, local_sem.at[BLOCKS])
    hid_copy.start()
    perm_copy = pltpu.make_async_copy(perm.at[core], perm_v, perm_sem)
    perm_copy.start()
    cot_copies = []
    for q in range(BLOCKS):
        copy = pltpu.make_async_copy(
            cot.at[:, pl.ds(q * WIDTH, WIDTH)], cot_v.at[q], local_sem.at[q]
        )
        cot_copies.append(copy)
    cot_copies[0].start()
    back_copy = pltpu.make_async_copy(back.at[core], back_v, local_sem.at[BLOCKS + 1])
    inputs = (
        (master, master_v),
        (codes1, codes_v.at[0]),
        (codes2, codes_v.at[1]),
        (cols1, cols_v.at[0]),
        (cols2, cols_v.at[1]),
        (rows1, rows1_s),
        (rows2, rows2_s),
        (step, step_s),
    )
    input_copies = [
        pltpu.make_async_copy(src, dst, input_sem.at[i]) for i, (src, dst) in enumerate(inputs)
    ]

    barrier = pltpu.get_barrier_semaphore()

    def greet(where):
        pl.semaphore_signal(barrier, inc=1, device_id=where, device_id_type=MESH)

    for distance in (2, -2, 1, -1):
        greet(on_ring(me + distance))
    for distance in (1, -1):
        across = at(me, lax.rem(other + distance + 8, 8))
        greet(across)
        greet({"dp_0": 1 - xl, **across})
    greet({"dp_0": 1 - xl})
    each_other(4, quad, lambda k: greet(in_quad(k)))

    def tell(i):
        for distance in (1, -1):
            pl.semaphore_signal(
                news.at[i],
                inc=1,
                device_id=at(me, lax.rem(other + distance + 8, 8)),
                device_id_type=MESH,
            )

    def hear(i):
        pl.semaphore_wait(news.at[i], 2)

    ring_copies = {}

    def send_ring(b, slot, distance, value):
        peak = jnp.maximum(jnp.max(jnp.abs(value), axis=0, keepdims=True), 1e-30)
        ship_scale[b, slot] = peak * (1.0 / TOP)
        coded = jnp.round(value * (TOP / peak))
        ship[b, slot] = coded.astype(I32).astype(I16)
        where = on_ring(me + distance)
        data = remote(
            ship.at[b, slot], land.at[b, slot], ring_send, ring_recv.at[b, slot], where
        )
        scale = remote(
            ship_scale.at[b, slot],
            land_scale.at[b, slot],
            scale_send,
            scale_recv.at[b, slot],
            where,
        )
        data.start()
        scale.start()
        ring_copies[b, slot] = (data, scale)

    def arrived(b, slot):
        data, scale = ring_copies[b, slot]
        data.wait_recv()
        scale.wait_recv()
        return land[b, slot].astype(I32).astype(F32) * land_scale[b, slot]

    def own(b, distance):
        return grad[b, NEED.index(distance)]

    def slots(b):
        return (0, 3) if long_way(b) > 0 else (3, 0)

    def first_sends(b):
        way = long_way(b)
        long, short = slots(b)
        send_ring(b, 6, way if steps_of(b) == 4 else 2 * way, own(b, 4))
        if steps_of(b) == 3:
            send_ring(b, long, way, own(b, 3 * way))
        send_ring(b, short, -way, own(b, -3 * way))

    hid_copy.wait()
    perm_copy.wait()
    for copy in (*cot_copies[1:], *input_copies, back_copy):
        copy.start()
    hid_t[...] = lax.dot_general(
        perm_v[...],
        hid_v[...],
        (((1,), (1,)), ((), ())),
        preferred_element_type=F32,
    ).astype(BF16)

    def multiply(b, first, last):
        lhs = jnp.concatenate(
            [
                hid_t[pl.ds(pl.multiple_of(lax.rem(me + d + 8, 8) * CHUNK, CHUNK), CHUNK)]
                for d in NEED[first:last]
            ],
            axis=0,
        )
        product = jnp.dot(lhs, cot_v[b], preferred_element_type=F32)
        grad[b, first:last] = product.reshape(last - first, CHUNK, WIDTH)

    for b in range(BLOCKS):
        cot_copies[b].wait()
        multiply(b, 0, FAR)
        if b == 0:
            pl.semaphore_wait(barrier, 4 + 4 + 1 + 3)
            tell(0)
        first_sends(b)
    for b in range(BLOCKS):
        multiply(b, FAR, RING)
    hear(0)
    tell(1)

    for b in range(BLOCKS):
        way = long_way(b)
        long, short = slots(b)
        far = arrived(b, 6)
        if steps_of(b) == 4:
            send_ring(b, long, way, far + own(b, 3 * way))
        else:
            send_ring(b, long + 1, way, far + arrived(b, long) + own(b, 2 * way))
        send_ring(b, short + 1, -way, arrived(b, short) + own(b, -2 * way))
    hear(1)
    tell(2)
    for b in range(BLOCKS):
        way = long_way(b)
        long, short = slots(b)
        if steps_of(b) == 4:
            send_ring(b, long + 1, way, arrived(b, long) + own(b, 2 * way))
        else:
            send_ring(b, long + 2, way, arrived(b, long + 1) + own(b, way))
        send_ring(b, short + 2, -way, arrived(b, short + 1) + own(b, -way))
    hear(2)
    for b in range(BLOCKS):
        if steps_of(b) == 3:
            continue
        way = long_way(b)
        long, _ = slots(b)
        send_ring(b, long + 2, way, arrived(b, long + 1) + own(b, way))
    for h in (1, 0):
        for i in range(2):
            b = 2 * h + i
            total[h, :, WIDTH * i : WIDTH * (i + 1)] = own(b, 0) + arrived(b, 2) + arrived(b, 5)
        value = total[h]
        peak = jnp.maximum(jnp.max(jnp.abs(value), axis=0, keepdims=True), 1e-30)
        power = jnp.floor(jnp.log2(peak)) + 1.0
        total[h] = jnp.round(value * (TOP * jnp.exp2(-power)))
        for k in range(PLANE):
            piece = jnp.concatenate([total[h, OWN * k : OWN * k + OWN], power], axis=0)
            piece_out[h, k] = piece.astype(I32).astype(I16)
        piece_in[h, place] = piece_out[h, place]

        def send_piece(k, h=h):
            remote(
                piece_out.at[h, k],
                piece_in.at[h, place],
                plane_send.at[h],
                plane_recv.at[h],
                in_plane(k),
            ).start()

        each_other(PLANE, place, send_piece)

    def as_column(ref):
        at = lax.broadcasted_iota(I32, (OWN, 1), 0)
        return jnp.where(at == 0, ref[0], jnp.where(at == 1, ref[1], ref[2]))

    for copy in input_copies:
        copy.wait()
    first_old = (
        (codes_v[0].astype(F32) - 7.5) / 7.5 * jnp.minimum(as_column(rows1_s), cols_v[0])
    )
    level = (codes_v[1].astype(F32) + 1.0) / 16.0
    second_old = level * level * jnp.minimum(as_column(rows2_s), cols_v[1])
    steps = jnp.full((1, 128), step_s[0].astype(F32))
    first_fix = (1.0 - jnp.exp(steps * np.float32(np.log(0.9))))[:, 0:1]
    second_fix = (1.0 - jnp.exp(steps * np.float32(np.log(0.95))))[:, 0:1]

    parts = {}
    for h in (1, 0):
        bytes_of(piece_in.at[h, pl.ds(0, PLANE - 1)], plane_recv.at[h])
        parts[h] = jnp.zeros((OWN, HALF), F32)
        for k in range(PLANE):
            piece = piece_in[h, k].astype(I32).astype(F32)
            unit = jnp.exp2(piece[OWN : OWN + 1]) * (1.0 / TOP)
            parts[h] = parts[h] + piece[0:OWN] * unit
    gradient = jnp.concatenate([parts[0], parts[1]], axis=1)

    square = jnp.sum(jnp.sum(gradient * gradient, axis=1, keepdims=True), axis=0, keepdims=True)
    square = jnp.broadcast_to(square, (1, 128))
    for phase, (count, mine, to) in enumerate(((16, column, in_column), (32, sheet, in_sheet))):
        norm_out[phase] = square
        norm_in[phase, mine] = square

        def send_norm(k, phase=phase, mine=mine, to=to):
            remote(
                norm_out.at[phase],
                norm_in.at[phase, mine],
                norm_send.at[phase],
                norm_recv.at[phase],
                to(k),
            ).start()

        each_other(count, mine, send_norm)
        bytes_of(norm_in.at[phase, pl.ds(0, count - 1)], norm_recv.at[phase])
        square = jnp.sum(norm_in[phase, 0:count], axis=0)

    entries = np.float32(3145728.0)
    limit = np.float32(0.01) * np.sqrt(entries)
    clipf = jnp.minimum(1.0, limit / (jnp.sqrt(square) + 1e-06))[:, 0:1]
    clipped = clipf * gradient
    first_new = 0.9 * first_old + 0.1 * clipped
    second_new = 0.95 * second_old + 0.05 * clipped * clipped
    ratio = first_new / first_fix / (jnp.sqrt(second_new / second_fix) + 1e-08)
    new_master = master_v[...] - 0.001 * (ratio + 0.1 * master_v[...])

    rounded = new_master.astype(BF16)
    fresh[...] = rounded
    near[place] = rounded
    each_other(
        PLANE,
        place,
        lambda k: remote(fresh, near.at[place], near_send, near_recv, in_plane(k)).start(),
    )

    results = (
        (result_v.at[0], out_master),
        (result_v.at[1], out_ratio),
        (result_v.at[2], out_scaled1),
        (result_v.at[3], out_scaled2),
        (row_result, out_rows),
        (col_result.at[0], out_cols1),
        (col_result.at[1], out_cols2),
    )
    result_copies = [
        pltpu.make_async_copy(src, dst, input_sem.at[i]) for i, (src, dst) in enumerate(results)
    ]
    result_v[0] = new_master
    result_v[1] = ratio
    result_copies[0].start()
    result_copies[1].start()

    first_abs = jnp.abs(first_new)
    row_out[0] = jnp.broadcast_to(jnp.max(first_abs, axis=1, keepdims=True), (OWN, 128))
    row_out[1] = jnp.broadcast_to(jnp.max(second_new, axis=1, keepdims=True), (OWN, 128))
    row_in[quad] = row_out[...]
    each_other(
        4,
        quad,
        lambda k: remote(row_out, row_in.at[quad], row_send, row_recv, in_quad(k)).start(),
    )
    tops = jnp.concatenate(
        [jnp.max(first_abs, axis=0, keepdims=True), jnp.max(second_new, axis=0, keepdims=True)],
        axis=0,
    )
    for k in range(PLANE):
        col_out[0, k] = tops[:, 128 * k : 128 * k + 128]
    col_in[0, place] = col_out[0, place]
    each_other(
        PLANE,
        place,
        lambda k: remote(
            col_out.at[0, k],
            col_in.at[0, place],
            col_send.at[0],
            col_recv.at[0],
            in_plane(k),
        ).start(),
    )

    whole_copies = {}

    def pass_on(b, slot, distance, c):
        at = lax.rem(c + 16, 8)
        copy = remote(
            whole.at[b, at],
            whole.at[b, at],
            whole_send,
            ring_recv.at[b, slot],
            on_ring(me + distance),
        )
        copy.start()
        whole_copies[b, slot] = copy

    bytes_of(near.at[pl.ds(0, PLANE - 1)], near_recv)
    for b in range(BLOCKS):
        for k in range(PLANE):
            join[b, OWN * k : OWN * k + OWN] = near[k, :, WIDTH * b : WIDTH * (b + 1)].astype(F32)
        whole[b, me] = join[b].astype(BF16)
        pass_on(b, 0, 1, me)
        pass_on(b, 3, -1, me)

    bytes_of(col_in.at[0, pl.ds(0, PLANE - 1)], col_recv.at[0])
    best = jnp.max(col_in[0], axis=0)
    col_out[1, 0] = best
    col_in[1, me] = best
    each_other(
        RING,
        me,
        lambda c: remote(
            col_out.at[1, 0], col_in.at[1, me], col_send.at[1], col_recv.at[1], on_ring(c)
        ).start(),
    )

    def step_on(s):
        for b in range(BLOCKS):
            way = long_way(b)
            for first, direction in ((0, 1), (3, -1)):
                whole_copies[b, first + s - 1].wait_recv()
                if s == 2 and direction == way and steps_of(b) == 3:
                    pass_on(b, 6, 2 * way, me - 2 * way)
                pass_on(b, first + s, direction, me - direction * s)

    step_on(1)
    step_on(2)

    bytes_of(col_in.at[1, pl.ds(0, 7)], col_recv.at[1])
    best = jnp.max(col_in[1, 0:8], axis=0)
    col_out[2, 0] = best
    col_in[2, place] = best
    each_other(
        PLANE,
        place,
        lambda k: remote(
            col_out.at[2, 0], col_in.at[2, place], col_send.at[2], col_recv.at[2], in_plane(k)
        ).start(),
    )
    bytes_of(row_in.at[pl.ds(0, 3)], row_recv)
    row_top = jnp.max(row_in[...], axis=0)
    row_result[...] = row_top
    result_copies[4].start()

    for b in range(BLOCKS):
        if steps_of(b) == 3:
            continue
        way = long_way(b)
        long, _ = slots(b)
        whole_copies[b, long + 2].wait_recv()
        pass_on(b, 6, way, me - 3 * way)

    back_copy.wait()
    out_copies = []
    for b in (2, 3, 0, 1):
        for slot in (2, 5, 6):
            if steps_of(b) == 3 or slot != slots(b)[0] + 2:
                whole_copies[b, slot].wait_recv()
        block = whole[b].reshape(ROWS, WIDTH)
        natural[b] = jnp.dot(back_v[...], block, preferred_element_type=F32).astype(BF16)
        copy = pltpu.make_async_copy(
            natural.at[b], out_natural.at[:, pl.ds(b * WIDTH, WIDTH)], local_sem.at[b]
        )
        copy.start()
        out_copies.append(copy)

    bytes_of(col_in.at[2, pl.ds(0, PLANE - 1)], col_recv.at[2])
    for k in range(PLANE):
        col_result[0, :, 128 * k : 128 * k + 128] = col_in[2, k, 0:1]
        col_result[1, :, 128 * k : 128 * k + 128] = col_in[2, k, 1:2]
    result_v[2] = first_new / (jnp.minimum(row_top[0, :, 0:1], col_result[0]) + 1e-08)
    result_v[3] = second_new / (jnp.minimum(row_top[1, :, 0:1], col_result[1]) + 1e-08)
    for i in (2, 3, 5, 6):
        result_copies[i].start()

    bytes_of(ship, ring_send)
    bytes_of(ship_scale, scale_send)
    bytes_of(whole.at[:, pl.ds(0, 7)], whole_send)
    for h in range(2):
        bytes_of(piece_out.at[h, pl.ds(0, PLANE - 1)], plane_send.at[h])
    for phase in range(2):
        bytes_of(norm_in.at[phase, pl.ds(0, 31 if phase else 15)], norm_send.at[phase])
    for phase in range(3):
        bytes_of(
            col_in.at[phase, pl.ds(0, 7 if phase == 1 else PLANE - 1)], col_send.at[phase]
        )
    bytes_of(near.at[pl.ds(0, PLANE - 1)], near_send)
    bytes_of(row_in.at[pl.ds(0, 3)], row_send)
    for copy in (*out_copies, *result_copies):
        copy.wait()


def finish(
    natural,
    master,
    ratio,
    scaled1,
    scaled2,
    rows,
    cols1,
    cols2,
    out_master,
    out_ratio,
    out_params,
    out_scaled1,
    out_scaled2,
    out_rows1,
    out_cols1,
    out_rows2,
    out_cols2,
    natural_v,
    own_v,
    col_v,
    row_v,
    row1_s,
    row2_s,
    big_sem,
    small_sem,
):
    moves = []
    for i in range(RING):
        at = pl.ds(i * CHUNK, CHUNK)
        moves.append((natural.at[at], natural_v.at[at], out_params.at[at], big_sem.at[i]))
    sources = (master, ratio, scaled1, scaled2)
    targets = (out_master, out_ratio, out_scaled1, out_scaled2)
    for i in range(4):
        moves.append((sources[i], own_v.at[i], targets[i], small_sem.at[i]))
    moves.append((cols1, col_v.at[0], out_cols1, small_sem.at[4]))
    moves.append((cols2, col_v.at[1], out_cols2, small_sem.at[5]))
    row_load = pltpu.make_async_copy(rows, row_v, small_sem.at[6])
    row_load.start()
    ins = [pltpu.make_async_copy(src, at, sem) for src, at, _, sem in moves]
    for copy in ins:
        copy.start()
    outs = []
    for load, (_, at, target, sem) in zip(ins, moves, strict=True):
        load.wait()
        copy = pltpu.make_async_copy(at, target, sem)
        copy.start()
        outs.append(copy)
    row_load.wait()
    for j in range(OWN):
        row1_s[j] = jnp.max(row_v[0, j : j + 1])
        row2_s[j] = jnp.max(row_v[1, j : j + 1])
    for i, (src, dst) in enumerate(((row1_s, out_rows1), (row2_s, out_rows2))):
        copy = pltpu.make_async_copy(src, dst, small_sem.at[6 + i])
        copy.start()
        outs.append(copy)
    for copy in outs:
        copy.wait()


def permutations():
    natural = np.arange(ROWS)
    by_y = natural.reshape(PLANE, RING, OWN).transpose(1, 0, 2).reshape(-1)
    by_z = natural.reshape(2, RING, RING, OWN).transpose(1, 0, 2, 3).reshape(-1)
    to_y = np.zeros((ROWS, ROWS), np.float32)
    to_y[natural, by_y] = 1.0
    to_z = np.zeros((ROWS, ROWS), np.float32)
    to_z[natural, by_z] = 1.0
    there = np.stack([to_z, to_y])
    return there, there.transpose(0, 2, 1)


def shards(
    hidden_input,
    output_cotangent,
    master_weights,
    first_codes,
    second_codes,
    first_rows,
    first_cols,
    second_rows,
    second_cols,
    step_count,
):
    own = jax.ShapeDtypeStruct((OWN, COLS), F32)
    row = jax.ShapeDtypeStruct((OWN,), F32)
    col = jax.ShapeDtypeStruct((1, COLS), F32)
    anywhere = pl.BlockSpec(memory_space=pl.ANY)
    hbm = pl.BlockSpec(memory_space=pltpu.HBM)
    dma = pltpu.SemaphoreType.DMA
    perm, back = (jnp.asarray(p, BF16) for p in permutations())
    new_master, ratio, natural, scaled1, scaled2, rows, cols1, cols2 = pl.pallas_call(
        kernel,
        out_shape=(
            own,
            own,
            jax.ShapeDtypeStruct((ROWS, COLS), BF16),
            own,
            own,
            jax.ShapeDtypeStruct((2, OWN, 128), F32),
            col,
            col,
        ),
        in_specs=[hbm] * 12,
        out_specs=(hbm,) * 8,
        scratch_shapes=[
            pltpu.VMEM((OWN, COLS), F32),
            pltpu.VMEM((2, OWN, COLS), I32),
            pltpu.VMEM((2, 1, COLS), F32),
            pltpu.SMEM((OWN,), F32),
            pltpu.SMEM((OWN,), F32),
            pltpu.SMEM((1,), I32),
            pltpu.VMEM((4, OWN, COLS), F32),
            pltpu.VMEM((2, OWN, 128), F32),
            pltpu.VMEM((2, 1, COLS), F32),
            pltpu.VMEM((TOKENS, ROWS), BF16),
            pltpu.VMEM((BLOCKS, TOKENS, WIDTH), BF16),
            pltpu.VMEM((ROWS, ROWS), BF16),
            pltpu.VMEM((ROWS, ROWS), BF16),
            pltpu.VMEM((ROWS, TOKENS), BF16),
            pltpu.VMEM((BLOCKS, RING, CHUNK, WIDTH), F32),
            pltpu.VMEM((BLOCKS, 7, CHUNK, WIDTH), I16),
            pltpu.VMEM((BLOCKS, 7, 1, WIDTH), F32),
            pltpu.VMEM((BLOCKS, 7, CHUNK, WIDTH), I16),
            pltpu.VMEM((BLOCKS, 7, 1, WIDTH), F32),
            pltpu.VMEM((2, CHUNK, HALF), F32),
            pltpu.VMEM((2, PLANE, OWN + 1, HALF), I16),
            pltpu.VMEM((2, PLANE, OWN + 1, HALF), I16),
            pltpu.VMEM((2, 1, 128), F32),
            pltpu.VMEM((2, 32, 1, 128), F32),
            pltpu.VMEM((OWN, COLS), BF16),
            pltpu.VMEM((PLANE, OWN, COLS), BF16),
            pltpu.VMEM((BLOCKS, CHUNK, WIDTH), F32),
            pltpu.VMEM((BLOCKS, RING, CHUNK, WIDTH), BF16),
            pltpu.VMEM((BLOCKS, ROWS, WIDTH), BF16),
            pltpu.VMEM((3, PLANE, 2, 128), F32),
            pltpu.VMEM((3, PLANE, 2, 128), F32),
            pltpu.VMEM((2, OWN, 128), F32),
            pltpu.VMEM((4, 2, OWN, 128), F32),
            pltpu.SemaphoreType.REGULAR((3,)),
            dma((8,)),
            dma((BLOCKS + 2,)),
            dma,
            dma,
            dma((BLOCKS, 7)),
            dma,
            dma((BLOCKS, 7)),
            dma((2,)),
            dma((2,)),
            dma((2,)),
            dma((2,)),
            dma,
            dma,
            dma,
            dma((3,)),
            dma((3,)),
            dma,
            dma,
        ],
        compiler_params=pltpu.CompilerParams(
            collective_id=0, has_side_effects=True, vmem_limit_bytes=60 * 1024 * 1024
        ),
    )(
        hidden_input,
        output_cotangent,
        master_weights,
        first_codes,
        second_codes,
        first_rows,
        first_cols.reshape(1, -1),
        second_rows,
        second_cols.reshape(1, -1),
        step_count.reshape(1),
        perm,
        back,
    )
    outs = pl.pallas_call(
        finish,
        out_shape=(
            own,
            own,
            jax.ShapeDtypeStruct((ROWS, COLS), BF16),
            own,
            own,
            row,
            col,
            row,
            col,
        ),
        in_specs=[anywhere] * 8,
        out_specs=(hbm,) * 9,
        scratch_shapes=[
            pltpu.VMEM((ROWS, COLS), BF16),
            pltpu.VMEM((4, OWN, COLS), F32),
            pltpu.VMEM((2, 1, COLS), F32),
            pltpu.VMEM((2, OWN, 128), F32),
            pltpu.SMEM((OWN,), F32),
            pltpu.SMEM((OWN,), F32),
            dma((RING,)),
            dma((8,)),
        ],
        compiler_params=pltpu.CompilerParams(vmem_limit_bytes=60 * 1024 * 1024),
    )(natural, new_master, ratio, scaled1, scaled2, rows, cols1, cols2)
    outs = list(outs)
    outs[6] = outs[6].reshape(-1)
    outs[8] = outs[8].reshape(-1)
    return tuple(outs)


def solution(mesh):
    finer = Mesh(mesh.devices.reshape(2, 8, 8, 2, 2), ("dp_0", "dp_1", "dp_2", "mp_0", "mp_1"))
    in_specs = (
        P(DP, None),
        P(DP, MP),
        P(DP, MP),
        P(DP, MP),
        P(DP, MP),
        P(DP),
        P(MP),
        P(DP),
        P(MP),
        P(),
    )
    out_specs = (
        P(DP, MP),
        P(DP, MP),
        P(None, MP),
        P(DP, MP),
        P(DP, MP),
        P(DP),
        P(MP),
        P(DP),
        P(MP),
    )
    return jax.shard_map(
        shards, mesh=finer, in_specs=in_specs, out_specs=out_specs, check_vma=False
    )
```
